32 devices in a mesh: dp: 4 (over x, core), mp: 8 (over z, y).
Axes of the slice: x: 2, y: 2, z: 4, core: 2. Of those that a mesh axis runs over, the one named last changes fastest.
Arguments:
- packed_token_rows: int32 [16, 1024], P('dp'), may hold values from 0 to 44799
- example_numbers: int32 [16, 1024], P('dp'), may hold values from 0 to 15, never falling along the last dimension, each value on 1 to 128 neighbouring positions
- completion: int32 [16, 1024], P('dp'), may hold values 0 or 1
- global_token_count: int32 [], replicated, may hold values from 4096 to 8191
- owners: int32 [4, 4], replicated, may hold values from 0 to 3
- optimizer_step: int32 [], replicated, may hold values from 1 to 20
- embedding: bfloat16 [51200, 1024], P('mp'), may hold values from -0.375 to 0.375
- positions: bfloat16 [1024, 1024], replicated, may hold values from -0.3984375 to 0.3984375
- gains: float32 [3, 1024], replicated, may hold values from 0.1 to 1.9
- query_key_value_weight: bfloat16 [1024, 3, 1024], P(None, None, 'mp'), may hold values from -0.1875 to 0.1875
- attention_output_weight: bfloat16 [1024, 1024], P('mp'), may hold values from -0.75 to 0.75
- feedforward_input_weight: bfloat16 [1024, 4096], P(None, 'mp'), may hold values from -0.1875 to 0.1875
- feedforward_output_weight: bfloat16 [1024, 4096], P(None, 'mp'), may hold values from -0.09375 to 0.09375
- adapter_down_weight: bfloat16 [2, 4, 1024], replicated, may hold values from -0.1875 to 0.1875
- adapter_up_weight: bfloat16 [2, 4, 1024], P(None, None, 'mp'), may hold values from -0.19921875 to 0.19921875
- master: float32 [4, 4, 1024], P(None, None, 'mp'), may hold values from -0.2 to 0.2
- first_moment: float32 [4, 4, 1024], P(None, None, 'mp'), may hold values from -0.006 to 0.006
- second_moment: float32 [4, 4, 1024], P(None, None, 'mp'), may hold values from 1e-08 to 1e-07
Outputs:
- completion_loss: float32 [], replicated
- grad_norm: float32 [], replicated
- new_first: float32 [4, 4, 4, 1024], P('dp', None, None, 'mp')
- new_second: float32 [4, 4, 4, 1024], P('dp', None, None, 'mp')
- new_master: float32 [4, 4, 4, 1024], P('dp', None, None, 'mp')
- new_copy: bfloat16 [4, 4, 4, 1024], P('dp', None, None, 'mp')
The draws below stay inside these ranges and needn't reach their ends.
Inputs may be any that keep to these rules, and one draw needn't show every extreme that they name: `example_numbers`: never falling along a row.
All inputs are finite; a program needn't handle non-finite values. No bound on the sum of `completion` on one device may be relied on, other than what follows from the above.
Results may differ from the reference program's by a relative error of at most 0.015.
Values may be sent and summed in bfloat16 or wider, within the bound.
A program may use at most 192 MiB of HBM per device.

```python
import math
from functools import partial
import jax
import jax.numpy as jnp
import numpy as np
from jax import lax

MODEL_WIDTH = 1024
HEADS = 16
HEAD_DIM = 64
FF = 4096
VOCAB = 51200
ADAPTER_RANK = 4
SEQ = 1024
BATCH = 16
N_DP = 4


def place_ends(array, own_key, smallest, high):
    shape = array.shape
    spot = [jax.random.randint(jax.random.fold_in(own_key, axis), (), 0, shape[axis]) for axis in range(len(shape))]
    array = array.at[tuple(spot)].set(smallest)
    longest = shape.index(max(shape))
    spot[longest] = (spot[longest] + 1) % shape[longest]
    return array.at[tuple(spot)].set(high)


def block_levels(key, extent, split, least, high):
    gain = 1.0
    for position, shards_of in split:
        draws = jax.random.uniform(jax.random.fold_in(jax.random.fold_in(key, 6), position), (shards_of,), jnp.float32, least / len(split), high / len(split))
        gain = gain * jnp.repeat(jnp.exp(draws), extent[position] // shards_of).reshape((-1,) + (1,) * (len(extent) - 1 - position))
    return gain


def cumulative_ranks(amount, skew):
    portions = [(1 << 20) // math.isqrt(rank ** skew) + 1 for rank in range(1, amount + 1)]
    scale = 1 + sum(portions) // (1 << 30)
    return np.cumsum(np.array([max(1, weight // scale) for weight in portions]))


def ranked(rng, extent, amount, lean):
    grid = cumulative_ranks(amount, lean)
    ticket = jax.random.randint(jax.random.fold_in(rng, 1), extent, 0, int(grid[amount - 1]))
    rank = jnp.searchsorted(jnp.asarray(grid, jnp.int32), ticket, side="right")
    return jax.random.permutation(jax.random.fold_in(rng, 2), amount)[rank].astype(jnp.int32)


def split_up(amount, total, most, slope):
    portions = [(1 << 20) // math.isqrt(rank ** slope) + 1 for rank in range(2, amount + 1)]
    spare, counts = total - most - (amount - 1), [1] * (amount - 1)
    while spare > 0:
        free = [i for i in range(amount - 1) if counts[i] < most]
        mass, budget = sum([portions[i] for i in free]), spare
        for i in free:
            more = min(most - counts[i], max(1, budget * portions[i] // mass), spare)
            counts[i] = counts[i] + more
            spare = spare - more
    return np.array([most] + counts)


def ragged_sizes(rng, amount, total, limit, skew):
    if amount == 2:
        one = jax.random.randint(rng, (), max(1, total - limit), min(limit, total - 1) + 1)
        return jnp.stack([one, total - one])
    lengths = jnp.asarray(split_up(amount, total, limit, skew), jnp.int32)
    twos = (amount - 1) // 2
    source_of, sink = lengths[1:1 + 2 * twos:2], lengths[2:2 + 2 * twos:2]
    margin = jnp.minimum(source_of - 1, limit - sink)
    shifted = jax.random.randint(jax.random.fold_in(rng, 1), (twos,), 0, 1 << 20) % (margin + 1)
    lengths = lengths.at[1:1 + 2 * twos:2].set(source_of - shifted).at[2:2 + 2 * twos:2].set(sink + shifted)
    return lengths[jax.random.permutation(jax.random.fold_in(rng, 2), amount)]


def bell_draw(own_key, dims, scale, reach, shards=(), kind=jnp.bfloat16):
    result = scale * jax.random.normal(own_key, dims, jnp.float32)
    if shards:
        result = result * block_levels(own_key, dims, shards, -0.22, 0.18)
    return jnp.clip(result, -reach, reach).astype(kind)


def setup_inputs(seed: int = 0) -> dict:
    streams_of = jax.random.split(jax.random.key(seed), 19)
    return {
        "packed_token_rows": place_ends(ranked(streams_of[0], (BATCH, SEQ), min(50257, VOCAB - VOCAB // 8), 2), jax.random.fold_in(streams_of[0], 3), 0, (min(50257, VOCAB - VOCAB // 8)) - 1).astype(jnp.int32),
        "example_numbers": jax.vmap(lambda own: jnp.searchsorted(jnp.cumsum(ragged_sizes(own, max(4, SEQ // 64), SEQ, max(16, SEQ // 8), 1)), jnp.arange(SEQ), side="right"))(jax.random.split(streams_of[1], BATCH)).reshape((BATCH, SEQ)).astype(jnp.int32),
        "completion": place_ends((jax.random.randint(streams_of[2], (BATCH, SEQ), 0, 2) < 1).astype(jnp.int32), jax.random.fold_in(streams_of[2], 1), 0, 1),
        "global_token_count": jax.random.randint(streams_of[3], (), BATCH * SEQ // 4, BATCH * SEQ // 2).astype(jnp.int32),
        "owners": place_ends(jax.random.randint(streams_of[4], (4, ADAPTER_RANK), 0, N_DP), jax.random.fold_in(streams_of[4], 1), 0, N_DP - 1).astype(jnp.int32),
        "optimizer_step": jax.random.randint(streams_of[5], (), 1, 21).astype(jnp.int32),
        "embedding": bell_draw(streams_of[6], (VOCAB, MODEL_WIDTH), (MODEL_WIDTH // 4) ** -0.5, 0.375, ((0, 8),)),
        "positions": bell_draw(streams_of[7], (SEQ, MODEL_WIDTH), 0.0625, 0.3984375),
        "gains": jnp.clip(1.0 + 0.18 * jax.random.normal(streams_of[8], (3, MODEL_WIDTH), jnp.float32), 0.1, 1.9),
        "query_key_value_weight": bell_draw(streams_of[9], (MODEL_WIDTH, 3, MODEL_WIDTH), MODEL_WIDTH ** -0.5, 0.1875, ((2, 8),)),
        "attention_output_weight": bell_draw(streams_of[10], (MODEL_WIDTH, MODEL_WIDTH), (MODEL_WIDTH // 16) ** -0.5, 0.75, ((0, 8),)),
        "feedforward_input_weight": bell_draw(streams_of[11], (MODEL_WIDTH, FF), MODEL_WIDTH ** -0.5, 0.1875, ((1, 8),)),
        "feedforward_output_weight": bell_draw(streams_of[12], (MODEL_WIDTH, FF), FF ** -0.5, 0.09375, ((1, 8),)),
        "adapter_down_weight": bell_draw(streams_of[13], (2, ADAPTER_RANK, MODEL_WIDTH), MODEL_WIDTH ** -0.5, 0.1875),
        "adapter_up_weight": bell_draw(streams_of[14], (2, ADAPTER_RANK, MODEL_WIDTH), 0.03, 0.19921875, ((2, 8),)),
        "master": bell_draw(streams_of[15], (4, ADAPTER_RANK, MODEL_WIDTH), 0.03, 0.2, ((2, 8),), jnp.float32),
        "first_moment": bell_draw(streams_of[16], (4, ADAPTER_RANK, MODEL_WIDTH), 0.001, 0.006, ((2, 8),), jnp.float32),
        "second_moment": jnp.clip(jnp.exp(math.log(1.0000000116860974e-07) - 2.3025851 * jax.random.uniform(streams_of[17], (4, ADAPTER_RANK, MODEL_WIDTH), jnp.float32) ** block_levels(streams_of[17], (4, ADAPTER_RANK, MODEL_WIDTH), ((2, 8),), -0.2, 0.2)), 9.99999993922529e-09, 1.0000000116860974e-07),
    }


HIGHEST = lax.Precision.HIGHEST
EPS_NORM = 1e-05
ADAPTER_SCALE = 8.0
SCORE_SCALE = 0.125
MASK_VALUE = -1e+30
CLIP_NORM = 1.0
BETA_ONE = 0.9
BETA_TWO = 0.999
LEARN_RATE = 0.01
WEIGHT_DECAY = 0.01
ADAM_EPS = 1e-08

@jax.custom_vjp
def low(v):
    return lax.optimization_barrier(v.astype(jnp.bfloat16)).astype(jnp.float32)

@jax.custom_vjp
def low_back(v):
    return v

def low_keep(v):
    return (low(v), None)

def low_pass(kept, grad):
    return (grad,)

def back_keep(v):
    return (v, None)

def back_low(kept, grad):
    return (low(grad),)
low.defvjp(low_keep, low_pass)
low_back.defvjp(back_keep, back_low)

def layer_norm(values, gain_row):
    center = values - lax.optimization_barrier(jnp.mean(values, axis=-1, keepdims=True))
    spread = lax.optimization_barrier(jnp.mean(center * center, axis=-1, keepdims=True))
    return center * lax.rsqrt(spread + EPS_NORM) * gain_row

def matrix_product_exact(left, right):
    return jnp.dot(left, right, precision=HIGHEST)

def head_block(table, block_pair):
    rows_in, targets, row_weight = block_pair
    logits = low_back(matrix_product_exact(rows_in, table.T))
    row_total = jax.nn.logsumexp(logits, axis=-1)
    picked = jnp.take_along_axis(logits, targets[:, None], axis=1)[:, 0]
    return jnp.sum(row_weight * (row_total - picked))

def sequence_loss(frozen, gains, down, up_matrix, tok_count, inputs):
    embed, posit, query_key_value_weight, attention_output_weight, feedforward_input_weight, feedforward_output_weight = frozen
    tok_ids, seg_ids, comp_row = inputs
    places = jnp.arange(SEQ, dtype=jnp.int32)
    x_zero = jnp.take(embed, tok_ids, axis=0) + posit
    normed = low(layer_norm(x_zero, gains[0]))
    projected_query_key_value = matrix_product_exact(normed, query_key_value_weight.reshape(MODEL_WIDTH, 3 * MODEL_WIDTH)).reshape(SEQ, 3, MODEL_WIDTH)
    reduced_rank_path = low(low_back(matrix_product_exact(normed, down.reshape(2 * ADAPTER_RANK, MODEL_WIDTH).T)))
    query_matrix = low(low_back(projected_query_key_value[:, 0] + ADAPTER_SCALE * matrix_product_exact(reduced_rank_path[:, :ADAPTER_RANK], up_matrix[0])))
    keys_all = low(projected_query_key_value[:, 1])
    value_matrix_whole = low(low_back(projected_query_key_value[:, 2] + ADAPTER_SCALE * matrix_product_exact(reduced_rank_path[:, ADAPTER_RANK:], up_matrix[1])))
    heads_of = lambda array_in: array_in.reshape(SEQ, HEADS, HEAD_DIM)
    scores = jnp.einsum('qhd,khd->hqk', heads_of(query_matrix), heads_of(keys_all), precision=HIGHEST) * SCORE_SCALE
    allowed = (places[None, :] <= places[:, None]) & (seg_ids[None, :] == seg_ids[:, None])
    scores = low_back(jnp.where(allowed[None], scores, MASK_VALUE))
    probs_all = low(jax.nn.softmax(scores, axis=-1))
    attn_mixed = jnp.einsum('hqk,khd->qhd', probs_all, heads_of(value_matrix_whole), precision=HIGHEST)
    attn_mixed = low(low_back(attn_mixed.reshape(SEQ, MODEL_WIDTH)))
    hidden_one = x_zero + low_back(matrix_product_exact(attn_mixed, attention_output_weight))
    normed_two = low(layer_norm(hidden_one, gains[1]))
    fc_inner = low_back(matrix_product_exact(normed_two, feedforward_input_weight))
    active = low(jax.nn.gelu(fc_inner, approximate=True))
    hidden_two = hidden_one + low_back(matrix_product_exact(active, feedforward_output_weight.T))
    final_rows = low(layer_norm(hidden_two, gains[2]))
    next_ids = jnp.roll(tok_ids, -1)
    is_valid = (places < SEQ - 1) & (jnp.roll(seg_ids, -1) == seg_ids) & (jnp.roll(comp_row, -1) == 1)
    row_weight = is_valid.astype(final_rows.dtype) / tok_count
    block_rows = min(512, SEQ)
    blocks = (final_rows.reshape(-1, block_rows, MODEL_WIDTH), next_ids.reshape(-1, block_rows), row_weight.reshape(-1, block_rows))
    return jnp.sum(lax.map(jax.checkpoint(partial(head_block, embed)), blocks))

def reference(packed_token_rows, example_numbers, completion, global_token_count, owners, optimizer_step, embedding, positions, gains, query_key_value_weight, attention_output_weight, feedforward_input_weight, feedforward_output_weight, adapter_down_weight, adapter_up_weight, master, first_moment, second_moment):
    frozen = tuple((member.astype(jnp.float32) for member in (embedding, positions, query_key_value_weight, attention_output_weight, feedforward_input_weight, feedforward_output_weight)))
    tok_count = global_token_count.astype(jnp.float32)

    def loss_overall(down, up_matrix):
        one_seq = jax.checkpoint(lambda inputs: sequence_loss(frozen, gains, down, up_matrix, tok_count, inputs))
        return jnp.sum(lax.map(one_seq, (packed_token_rows, example_numbers, completion)))
    completion_loss, backward_product = jax.vjp(loss_overall, adapter_down_weight.astype(jnp.float32), adapter_up_weight.astype(jnp.float32))
    grad_down, gradient_up_matrix = backward_product(jnp.ones_like(completion_loss))
    grads = jnp.concatenate([grad_down, gradient_up_matrix], axis=0)
    grad_norm = jnp.sqrt(jnp.sum(grads * grads))
    clipped = grads * jnp.minimum(1.0, CLIP_NORM / (grad_norm + 1e-06))
    new_first = BETA_ONE * first_moment + (1.0 - BETA_ONE) * clipped
    new_second = BETA_TWO * second_moment + (1.0 - BETA_TWO) * clipped * clipped
    step_float = optimizer_step.astype(jnp.float32)
    first_hat = new_first / (1.0 - jnp.power(BETA_ONE, step_float))
    second_hat = new_second / (1.0 - jnp.power(BETA_TWO, step_float))
    new_weight = master - LEARN_RATE * (first_hat / (jnp.sqrt(second_hat) + ADAM_EPS) + WEIGHT_DECAY * master)
    owner_slots = (owners[None, :, :] == jnp.arange(N_DP, dtype=jnp.int32)[:, None, None]).astype(new_weight.dtype)
    slot_mask = owner_slots[:, :, :, None]
    return (completion_loss, grad_norm, slot_mask * new_first[None], slot_mask * new_second[None], slot_mask * new_weight[None], (slot_mask * new_weight[None]).astype(jnp.bfloat16))
```

```python
import functools

import jax
import jax.numpy as jnp
from jax import lax
from jax.experimental import pallas as pl
from jax.experimental.pallas import tpu as pltpu
from jax.sharding import PartitionSpec as P

HEAD_DIM = 64
EPS_NORM = 1e-05
ADAPTER_SCALE = 8.0
SCORE_SCALE = 0.125
MASK_VALUE = -1e30
CLIP_NORM = 1.0
BETA_ONE = 0.9
BETA_TWO = 0.999
LEARN_RATE = 0.01
WEIGHT_DECAY = 0.01
ADAM_EPS = 1e-08
HALO = 128
PAIR = 128
NT = (((1,), (1,)), ((), ()))
TN = (((0,), (0,)), ((), ()))
MESH = pl.DeviceIdType.MESH
VMEM_CAP = 62 * 2**20
LINE = 4
SIDE = 2


def is_own_mesh():
    return lax.axis_size("dp") == 4 and lax.axis_size("mp") == LINE * SIDE


def here():
    dp, mp = lax.axis_index("dp"), lax.axis_index("mp")
    return dp // 2, dp % 2, mp // SIDE, mp % SIDE


def dev(x, core, line, side):
    return {"dp": x * 2 + core, "mp": line * SIDE + side}


def greet(peers):
    barrier = pltpu.get_barrier_semaphore()
    for peer in peers:
        pl.semaphore_signal(barrier, inc=1, device_id=peer, device_id_type=MESH)
    pl.semaphore_wait(barrier, len(peers))


def greet_line(x, core, line, side, others):
    barrier = pltpu.get_barrier_semaphore()
    for peer in others:
        pl.semaphore_signal(barrier, inc=1, device_id=peer, device_id_type=MESH)

    @pl.when(line > 0)
    def _():
        pl.semaphore_signal(barrier, inc=1, device_id=dev(x, core, line - 1, side), device_id_type=MESH)

    @pl.when(line < LINE - 1)
    def _():
        pl.semaphore_signal(barrier, inc=1, device_id=dev(x, core, line + 1, side), device_id_type=MESH)

    inner = (line > 0) & (line < LINE - 1)

    @pl.when(inner)
    def _():
        pl.semaphore_wait(barrier, len(others) + 2)

    @pl.when(jnp.logical_not(inner))
    def _():
        pl.semaphore_wait(barrier, len(others) + 1)


def remote(src, dst, send_sem, recv_sem, peer):
    return pltpu.make_async_remote_copy(
        src_ref=src, dst_ref=dst, send_sem=send_sem, recv_sem=recv_sem, device_id=peer, device_id_type=MESH
    )


def swap_kernel(per_peer, src, dst, own_sem, send_sem, recv_sem):
    dp, mp = lax.axis_index("dp"), lax.axis_index("mp")
    count = LINE * SIDE
    peers = [{"dp": dp, "mp": lax.rem(mp + k, count)} for k in range(1, count)]
    greet(peers)
    copies = []
    for k in range(1, count):
        block = src.at[lax.rem(mp + k, count)] if per_peer else src
        copy = remote(block, dst.at[mp], send_sem.at[k], recv_sem.at[k], peers[k - 1])
        copy.start()
        copies.append(copy)
    own = pltpu.make_async_copy(src.at[mp] if per_peer else src, dst.at[mp], own_sem)
    own.start()
    own.wait()
    for copy in copies:
        copy.wait()


def swap(array, per_peer, collective):
    count = LINE * SIDE
    shape = array.shape if per_peer else (count,) + array.shape
    return pl.pallas_call(
        functools.partial(swap_kernel, per_peer),
        out_shape=jax.ShapeDtypeStruct(shape, array.dtype),
        in_specs=[pl.BlockSpec(memory_space=pltpu.VMEM)],
        out_specs=pl.BlockSpec(memory_space=pltpu.VMEM),
        scratch_shapes=[
            pltpu.SemaphoreType.DMA,
            pltpu.SemaphoreType.DMA((count,)),
            pltpu.SemaphoreType.DMA((count,)),
        ],
        compiler_params=pltpu.CompilerParams(
            collective_id=collective, has_side_effects=True, vmem_limit_bytes=VMEM_CAP
        ),
        name=f"swap_{collective}",
    )(array)


def agree_kernel(src, out, got, send_sem, recv_sem):
    dp, mp = lax.axis_index("dp"), lax.axis_index("mp")
    peers = [{"dp": lax.rem(dp + k, 4), "mp": mp} for k in range(1, 4)]
    greet(peers)
    copies = []
    for k in range(1, 4):
        copy = remote(src, got.at[k - 1], send_sem.at[k - 1], recv_sem.at[k - 1], peers[k - 1])
        copy.start()
        copies.append(copy)
    for copy in copies:
        copy.wait()
    out[...] = jnp.maximum(jnp.maximum(src[...], got[0]), jnp.maximum(got[1], got[2]))


def agree(values, collective):
    if not is_own_mesh():
        return lax.pmax(values, "dp")
    tile = jnp.zeros((8, 128), jnp.float32).at[0, : values.shape[0]].set(values)
    out = pl.pallas_call(
        agree_kernel,
        out_shape=jax.ShapeDtypeStruct((8, 128), jnp.float32),
        in_specs=[pl.BlockSpec(memory_space=pltpu.VMEM)],
        out_specs=pl.BlockSpec(memory_space=pltpu.VMEM),
        scratch_shapes=[
            pltpu.VMEM((3, 8, 128), jnp.float32),
            pltpu.SemaphoreType.DMA((3,)),
            pltpu.SemaphoreType.DMA((3,)),
        ],
        compiler_params=pltpu.CompilerParams(collective_id=collective, has_side_effects=True),
        name="agree",
    )(tile)
    return out[0, : values.shape[0]]


def weight_events(sizes):
    events, start = [], 0.0
    for k, size in enumerate(sizes):
        events.append((start - 1.5 * size - 0.001 if k else -1.0, "own", k, 0))
        for step in range(LINE):
            arrive = start + size * min(step, 2.5)
            if step:
                events.append((arrive, "line", k, step))
            events.append((arrive + 0.6 * size, "side", k, step))
            events.append((arrive + 1.2 * size, "x", k, step))
        start += 2.5 * size
    return sorted(events)


def weight_kernel(sizes, *refs):
    n = len(sizes)
    src, own_vmem, full = refs[:n], refs[n : 2 * n], refs[2 * n : 3 * n]
    own_sem = refs[3 * n]
    line_s, line_r, side_s, side_r, x_s, x_r, xf_s, xf_r, sib_s, sib_r, sib2_s, sib2_r, sib3_s, sib3_r = refs[3 * n + 1 :]
    x, core, line, side = here()
    up, down = dev(x, core, line + 1, side), dev(x, core, line - 1, side)
    across, twin, sibling = dev(x, core, line, 1 - side), dev(1 - x, core, line, side), dev(x, 1 - core, line, side)
    greet_line(x, core, line, side, [across, twin, sibling])
    mine = line * SIDE + side

    def piece(k, block, c, h):
        rows = full[k].shape[1]
        if h is None:
            return full[k].at[block, pl.ds(c * (rows // 2), rows // 2)]
        return full[k].at[block, pl.ds((c * 2 + h) * (rows // 4), rows // 4)]

    def own_piece(k, c, h):
        rows = full[k].shape[1]
        if h is None:
            return src[k].at[pl.ds(c * (rows // 2), rows // 2)]
        return src[k].at[pl.ds((c * 2 + h) * (rows // 4), rows // 4)]

    pending = []

    def when(cond, action):
        if cond is None:
            action()
        else:
            pl.when(cond)(action)

    def send(cond, src_ref, dst_ref, ssem, rsem, peer):
        copy = remote(src_ref, dst_ref, ssem, rsem, peer)
        when(cond, copy.start)
        pending.append((cond, copy))

    def arrived(cond, dst_ref, ssem, rsem):
        when(cond, remote(dst_ref, dst_ref, ssem, rsem, across).wait_recv)

    def exists(direction, step):
        if step == 0:
            return None
        return line >= step if direction == 0 else line + step < LINE

    def block_line(direction, step):
        return line - step if direction == 0 else line + step

    def flows(step):
        return (0,) if step == 0 else (0, 1)

    def both(first, second):
        return second if first is None else (first if second is None else first & second)

    def pass_on(k, step):
        for direction in flows(step):
            cond = exists(direction, step)
            block = block_line(direction, step) * SIDE + side
            far = step == LINE - 1
            whole = own_piece(k, core, None) if step == 0 else piece(k, block, core, None)
            part = own_piece(k, core, x) if step == 0 else piece(k, block, core, x)
            for way in (0, 1) if step == 0 else (direction,):
                if step < LINE - 1:
                    ok = both(cond, line < LINE - 1 if way == 0 else line > 0)
                    last = step + 1 == LINE - 1
                    send(
                        ok,
                        part if last else whole,
                        piece(k, block, core, x if last else None),
                        line_s.at[k, way, step],
                        line_r.at[k, way, step],
                        up if way == 0 else down,
                    )
            send(cond, part, piece(k, block, core, x), side_s.at[k, direction, step], side_r.at[k, direction, step], across)
            if far:
                send(cond, part, piece(k, block, core, x), xf_s.at[k, direction], xf_r.at[k, direction], twin)
            if step:
                send(
                    cond,
                    part if far else whole,
                    piece(k, block, core, x if far else None),
                    sib_s.at[k, direction, step],
                    sib_r.at[k, direction, step],
                    sibling,
                )

    for k in range(n):
        pltpu.make_async_copy(own_vmem[k], full[k].at[mine], own_sem.at[k]).start()

    for _, kind, k, step in weight_events(sizes):
        if kind == "own":
            pass_on(k, 0)
            continue
        for direction in flows(step):
            cond = exists(direction, step)
            near = block_line(direction, step) * SIDE + side
            other = block_line(direction, step) * SIDE + 1 - side
            far = step == LINE - 1
            if kind == "line":
                arrived(
                    cond,
                    piece(k, near, core, x if far else None),
                    line_s.at[k, direction, step - 1],
                    line_r.at[k, direction, step - 1],
                )
            elif kind == "side":
                part = piece(k, other, core, x)
                arrived(cond, part, side_s.at[k, direction, step], side_r.at[k, direction, step])
                send(cond, part, part, x_s.at[k, direction, step], x_r.at[k, direction, step], twin)
                send(cond, part, part, sib2_s.at[k, direction, step], sib2_r.at[k, direction, step], sibling)
            else:
                part = piece(k, other, core, 1 - x)
                arrived(cond, part, x_s.at[k, direction, step], x_r.at[k, direction, step])
                send(cond, part, part, sib3_s.at[k, direction, step], sib3_r.at[k, direction, step], sibling)
                if far:
                    part = piece(k, near, core, 1 - x)
                    arrived(cond, part, xf_s.at[k, direction], xf_r.at[k, direction])
                    send(cond, part, part, sib_s.at[k, direction, 0], sib_r.at[k, direction, 0], sibling)
        if kind == "line":
            pass_on(k, step)

    other_core = 1 - core
    for k in range(n):
        for step in range(LINE):
            for direction in flows(step):
                cond = exists(direction, step)
                near = block_line(direction, step) * SIDE + side
                other = block_line(direction, step) * SIDE + 1 - side
                far = step == LINE - 1
                if step:
                    arrived(
                        cond,
                        piece(k, near, other_core, x if far else None),
                        sib_s.at[k, direction, step],
                        sib_r.at[k, direction, step],
                    )
                if far:
                    arrived(cond, piece(k, near, other_core, 1 - x), sib_s.at[k, direction, 0], sib_r.at[k, direction, 0])
                arrived(cond, piece(k, other, other_core, x), sib2_s.at[k, direction, step], sib2_r.at[k, direction, step])
                arrived(cond, piece(k, other, other_core, 1 - x), sib3_s.at[k, direction, step], sib3_r.at[k, direction, step])
    for cond, copy in pending:
        when(cond, copy.wait_send)
    for k in range(n):
        pltpu.make_async_copy(own_vmem[k], full[k].at[mine], own_sem.at[k]).wait()


def gather_weights(blocks, collective):
    if not is_own_mesh():
        return [lax.all_gather(block, "mp", axis=0) for block in blocks]
    n = len(blocks)
    total = sum(block.size for block in blocks)
    sizes = [block.size / total for block in blocks]
    grid = pltpu.SemaphoreType.DMA((n, 2, LINE))
    pair = pltpu.SemaphoreType.DMA((n, 2))
    return pl.pallas_call(
        functools.partial(weight_kernel, sizes),
        out_shape=[jax.ShapeDtypeStruct((LINE * SIDE,) + block.shape, block.dtype) for block in blocks],
        in_specs=[pl.BlockSpec(memory_space=pl.ANY)] * n + [pl.BlockSpec(memory_space=pltpu.VMEM)] * n,
        out_specs=[pl.BlockSpec(memory_space=pl.ANY)] * n,
        scratch_shapes=[pltpu.SemaphoreType.DMA((n,)), grid, grid, grid, grid, grid, grid, pair, pair]
        + [grid] * 6,
        compiler_params=pltpu.CompilerParams(
            collective_id=collective, has_side_effects=True, vmem_limit_bytes=VMEM_CAP
        ),
        name="gather_weights",
    )(*blocks, *blocks)


def spread_kernel(own, out, own_sem, line_s, line_r, side_s, side_r):
    x, core, line, side = here()
    across = dev(x, core, line, 1 - side)
    greet_line(x, core, line, side, [across])
    up, down = dev(x, core, line + 1, side), dev(x, core, line - 1, side)
    mine = line * SIDE + side
    local = pltpu.make_async_copy(own, out.at[mine], own_sem)
    local.start()
    pending = []

    def send(cond, src, block, ssem, rsem, peer):
        copy = remote(src, out.at[block], ssem, rsem, peer)
        if cond is None:
            copy.start()
        else:
            pl.when(cond)(copy.start)
        pending.append((cond, copy))

    send(line < LINE - 1, own, mine, line_s.at[0, 0], line_r.at[0, 0], up)
    send(line > 0, own, mine, line_s.at[1, 0], line_r.at[1, 0], down)
    send(None, own, mine, side_s.at[0, 0], side_r.at[0, 0], across)
    for step in range(1, LINE):
        for way in (0, 1):
            cond = line >= step if way == 0 else line + step < LINE
            block = (line - step if way == 0 else line + step) * SIDE + side
            pl.when(cond)(
                remote(out.at[block], out.at[block], line_s.at[way, step - 1], line_r.at[way, step - 1], across).wait_recv
            )
            if step < LINE - 1:
                more = cond & (line < LINE - 1 if way == 0 else line > 0)
                send(more, out.at[block], block, line_s.at[way, step], line_r.at[way, step], up if way == 0 else down)
            send(cond, out.at[block], block, side_s.at[way, step], side_r.at[way, step], across)
    for step in range(LINE):
        for way in (0,) if step == 0 else (0, 1):
            cond = line >= step if way == 0 else line + step < LINE
            block = (line - step if way == 0 else line + step) * SIDE + 1 - side
            pl.when(cond)(
                remote(out.at[block], out.at[block], side_s.at[way, step], side_r.at[way, step], across).wait_recv
            )
    for cond, copy in pending:
        if cond is None:
            copy.wait_send()
        else:
            pl.when(cond)(copy.wait_send)
    local.wait()


def spread(rows, collective):
    if not is_own_mesh():
        return lax.all_gather(rows, "mp", axis=0)
    sems = pltpu.SemaphoreType.DMA((2, LINE))
    return pl.pallas_call(
        spread_kernel,
        out_shape=jax.ShapeDtypeStruct((LINE * SIDE,) + rows.shape, rows.dtype),
        in_specs=[pl.BlockSpec(memory_space=pltpu.VMEM)],
        out_specs=pl.BlockSpec(memory_space=pl.ANY),
        scratch_shapes=[pltpu.SemaphoreType.DMA, sems, sems, sems, sems],
        compiler_params=pltpu.CompilerParams(
            collective_id=collective, has_side_effects=True, vmem_limit_bytes=VMEM_CAP
        ),
        name=f"spread_{collective}",
    )(rows)


def collect_order(line, step):
    mirror = line // 2
    near = line * (1 - mirror) + (LINE - 1 - line) * mirror
    place = (LINE - 1, LINE - 2, 1 - near, near)[step]
    return place * (1 - mirror) + (LINE - 1 - place) * mirror


def collect_kernel(src, out, side_got, line_out, line_got, side_s, side_r, line_s, line_r):
    x, core, line, side = here()
    across = dev(x, core, line, 1 - side)
    greet_line(x, core, line, side, [across])
    up, down = dev(x, core, line + 1, side), dev(x, core, line - 1, side)
    copies = []
    for step in range(LINE):
        dest = collect_order(line, step)
        copy = remote(
            src.at[dest * SIDE + 1 - side], side_got.at[step], side_s.at[step], side_r.at[step], across
        )
        copy.start()
        copies.append(copy)

    def add(target, more):
        target[...] = (target[...].astype(jnp.float32) + more[...].astype(jnp.float32)).astype(target.dtype)

    for step in range(LINE):
        dest = collect_order(line, step)
        copies[step].wait_recv()
        partial = line_out.at[step]
        partial[...] = (
            src[dest * SIDE + side].astype(jnp.float32) + side_got[step].astype(jnp.float32)
        ).astype(partial.dtype)
        for way in (0, 1):
            behind = line > 0 if way == 0 else line < LINE - 1
            onward = dest >= line if way == 0 else dest <= line

            @pl.when(behind & onward)
            def _():
                got = line_got.at[way, dest]
                remote(got, got, line_s.at[way, step], line_r.at[way, dest], across).wait_recv()
                add(partial, got)

        for way in (0, 1):
            onward = dest > line if way == 0 else dest < line

            @pl.when(onward)
            def _():
                remote(
                    partial, line_got.at[way, dest], line_s.at[way, step], line_r.at[way, dest], up if way == 0 else down
                ).start()

    out[...] = line_out[LINE - 1]
    for step in range(LINE):
        dest = collect_order(line, step)
        copies[step].wait_send()
        for way in (0, 1):

            @pl.when(dest > line if way == 0 else dest < line)
            def _():
                remote(
                    line_out.at[step], line_got.at[way, dest], line_s.at[way, step], line_r.at[way, dest], across
                ).wait_send()


def collect(parts, collective):
    if not is_own_mesh():
        return lax.psum_scatter(parts, "mp", scatter_dimension=0)
    shape = parts.shape[1:]
    sems = pltpu.SemaphoreType.DMA((LINE,))
    pairs = pltpu.SemaphoreType.DMA((2, LINE))
    return pl.pallas_call(
        collect_kernel,
        out_shape=jax.ShapeDtypeStruct(shape, parts.dtype),
        in_specs=[pl.BlockSpec(memory_space=pltpu.VMEM)],
        out_specs=pl.BlockSpec(memory_space=pltpu.VMEM),
        scratch_shapes=[
            pltpu.VMEM((LINE,) + shape, parts.dtype),
            pltpu.VMEM((LINE,) + shape, parts.dtype),
            pltpu.VMEM((2, LINE) + shape, parts.dtype),
            sems,
            sems,
            pairs,
            pairs,
        ],
        compiler_params=pltpu.CompilerParams(
            collective_id=collective, has_side_effects=True, vmem_limit_bytes=VMEM_CAP
        ),
        name=f"collect_{collective}",
    )(parts)


def head_kernel(tile, tiles, x_ref, target_ref, table_ref, grad_ref, total_ref, logit_scr, acc):
    rows = x_ref.shape[0]
    target = target_ref[...]

    def table_rows(t):
        return table_ref[pl.ds(pl.multiple_of(t * tile, tile), tile), :]

    def logits(t):
        return lax.dot_general(x_ref[...], table_rows(t), NT, preferred_element_type=jnp.float32)

    logit_scr[0] = logits(0)
    acc[...] = jnp.zeros_like(acc)

    def lap(t, carry):
        peak, total = carry
        slot = t % 2

        @pl.when(t + 1 < tiles)
        def _():
            logit_scr[1 - slot] = logits(t + 1)

        scores = logit_scr[slot]
        new_peak = jnp.maximum(peak, jnp.max(scores, axis=-1, keepdims=True))
        prob = jnp.exp(scores - new_peak)
        shrink = jnp.exp(peak - new_peak)
        total = total * shrink + jnp.sum(prob, axis=-1, keepdims=True)
        column = lax.broadcasted_iota(jnp.int32, scores.shape, 1) + t * tile
        others = jnp.where(column == target, 0.0, prob).astype(jnp.bfloat16)
        acc[...] = acc[...] * shrink + jnp.dot(others, table_rows(t), preferred_element_type=jnp.float32)
        return new_peak, total

    start = (jnp.full((rows, 1), MASK_VALUE, jnp.float32), jnp.zeros((rows, 1), jnp.float32))
    peak, total = lax.fori_loop(0, tiles, lap, start)
    grad_ref[...] = acc[...] / total
    total_ref[...] = jnp.broadcast_to(peak + jnp.log(total), total_ref.shape)


def largest_block(extent, choices):
    for choice in choices:
        if extent % choice == 0:
            return choice
    return extent


def head(rows_in, target, table):
    count, width = rows_in.shape
    vocab = table.shape[0]
    tile = largest_block(vocab, (1280, 640, 256, 128))
    rows = largest_block(count, (384, 512, 256, 128))
    return pl.pallas_call(
        functools.partial(head_kernel, tile, vocab // tile),
        out_shape=(
            jax.ShapeDtypeStruct((count, width), jnp.float32),
            jax.ShapeDtypeStruct((count, 128), jnp.float32),
        ),
        grid=(count // rows,),
        in_specs=[
            pl.BlockSpec((rows, width), lambda i: (i, 0)),
            pl.BlockSpec((rows, 1), lambda i: (i, 0)),
            pl.BlockSpec((vocab, width), lambda i: (0, 0), pipeline_mode=pl.Buffered(1)),
        ],
        out_specs=(
            pl.BlockSpec((rows, width), lambda i: (i, 0)),
            pl.BlockSpec((rows, 128), lambda i: (i, 0)),
        ),
        scratch_shapes=[pltpu.VMEM((2, rows, tile), jnp.float32), pltpu.VMEM((rows, width), jnp.float32)],
        compiler_params=pltpu.CompilerParams(vmem_limit_bytes=VMEM_CAP),
        name=f"head_{count}",
    )(rows_in, target, table)


def norm_parts(values):
    center = values - jnp.mean(values, axis=-1, keepdims=True)
    spread_of = jnp.mean(center * center, axis=-1, keepdims=True)
    scale = lax.rsqrt(spread_of + EPS_NORM)
    return center * scale, scale


def layer_norm(values, gain_row):
    return norm_parts(values)[0] * gain_row


def norm_back(values, gain_row, grad_out):
    hat, scale = norm_parts(values)
    inner = grad_out * gain_row
    return scale * (
        inner
        - jnp.mean(inner, axis=-1, keepdims=True)
        - hat * jnp.mean(inner * hat, axis=-1, keepdims=True)
    )


GELU_A = 0.7978845608028654
GELU_B = 0.044715


def gelu(z):
    return 0.5 * z * (1.0 + jnp.tanh(GELU_A * (z + GELU_B * z * z * z)))


def gelu_slope(z):
    square = z * z
    curve = jnp.tanh(GELU_A * z * (1.0 + GELU_B * square))
    return 0.5 * (1.0 + curve) + 0.5 * z * (1.0 - curve * curve) * GELU_A * (1.0 + 3.0 * GELU_B * square)


def row_blocks(count, body, block=128):
    def lap(i, carry):
        body(pl.ds(pl.multiple_of(i * block, block), block))
        return carry

    lax.fori_loop(0, count // block, lap, 0)


def allowed_keys(seg_col, seg_row, block):
    rows = seg_col[HALO + block * PAIR : HALO + (block + 1) * PAIR, :]
    keys = seg_row[:, block * PAIR : block * PAIR + 2 * PAIR]
    shape = (PAIR, 2 * PAIR)
    causal = lax.broadcasted_iota(jnp.int32, shape, 1) <= lax.broadcasted_iota(jnp.int32, shape, 0) + HALO
    return causal & (rows == keys)


def head_lanes(shape, which):
    lane = lax.broadcasted_iota(jnp.int32, shape, 1)
    return lane < HEAD_DIM if which == 0 else lane >= HEAD_DIM


def only_head(values, which):
    return jnp.where(head_lanes(values.shape, which), values, jnp.zeros_like(values))


def probs_of(query, keys, which, allowed):
    scores = lax.dot_general(only_head(query, which), keys, NT, preferred_element_type=jnp.float32) * SCORE_SCALE
    scores = jnp.where(allowed, scores, MASK_VALUE)
    exp_blk = jnp.exp(scores - jnp.max(scores, axis=-1, keepdims=True))
    return exp_blk / jnp.sum(exp_blk, axis=-1, keepdims=True)


def forward_kernel(
    emb,
    pos,
    seg_col,
    seg_row,
    rank_row,
    gains,
    down,
    up_query,
    up_value,
    wq_hbm,
    wo_hbm,
    w1_hbm,
    w2_hbm,
    rows_out,
    pick_out,
    normed_out,
    low_out,
    query_out,
    key_out,
    value_out,
    one_out,
    two_out,
    fc_out,
    wq,
    wo,
    w1,
    w2,
    wide,
    attn,
    normed_two,
    fc_buf,
    wq_sem,
    w_sem,
    fc_sem,
):
    tokens = two_out.shape[0]
    reach = HALO + tokens
    pairs = query_out.shape[0]
    chunks = w1.shape[0]
    loads = []
    for p in range(pairs):
        loads.append(
            pltpu.make_async_copy(
                wq_hbm.at[p, pl.ds(0, wq.shape[1])], wq.at[p // 2, :, pl.ds((p % 2) * 3 * PAIR, 3 * PAIR)], wq_sem.at[p]
            )
        )
    others = [
        pltpu.make_async_copy(a, b, w_sem.at[i]) for i, (a, b) in enumerate(((wo_hbm, wo), (w1_hbm, w1), (w2_hbm, w2)))
    ]
    for load in loads + others:
        load.start()

    def first(rows):
        x_zero = emb[rows, :].astype(jnp.float32) + pos[rows, :].astype(jnp.float32)
        wide[rows, :] = x_zero
        normed_out[rows, :] = layer_norm(x_zero, gains[0:1, :]).astype(jnp.bfloat16)

    row_blocks(reach, first)
    low_out[...] = lax.dot_general(normed_out[...], down[...], NT, preferred_element_type=jnp.float32).astype(
        jnp.bfloat16
    )
    for load in loads:
        load.wait()

    def project(j, carry):
        both = jnp.dot(normed_out[...], wq[j], preferred_element_type=jnp.float32)
        for half in range(2):
            p = 2 * j + half
            cols = pl.ds(pl.multiple_of(p * PAIR, PAIR), PAIR)
            base = half * 3 * PAIR
            term_q = jnp.dot(low_out[HALO:, :], up_query[:, cols], preferred_element_type=jnp.float32)
            term_v = jnp.dot(low_out[...], up_value[:, cols], preferred_element_type=jnp.float32)
            query_out[p] = (both[HALO:, base : base + PAIR] + term_q).astype(jnp.bfloat16)
            key_out[p] = both[:, base + PAIR : base + 2 * PAIR].astype(jnp.bfloat16)
            value_out[p] = (both[:, base + 2 * PAIR : base + 3 * PAIR] + term_v).astype(jnp.bfloat16)
        return carry

    lax.fori_loop(0, pairs // 2, project, 0)

    def attend(p, carry):
        cols = pl.ds(pl.multiple_of(p * PAIR, PAIR), PAIR)
        for block in range(tokens // PAIR):
            allowed = allowed_keys(seg_col, seg_row, block)
            rows = slice(block * PAIR, (block + 1) * PAIR)
            window = slice(block * PAIR, block * PAIR + 2 * PAIR)
            query, keys, values = query_out[p, rows, :], key_out[p, window, :], value_out[p, window, :]
            mixed = [
                jnp.dot(probs_of(query, keys, h, allowed).astype(jnp.bfloat16), values, preferred_element_type=jnp.float32)
                for h in range(2)
            ]
            attn[rows, cols] = jnp.where(head_lanes(mixed[0].shape, 0), mixed[0], mixed[1]).astype(jnp.bfloat16)
        return carry

    lax.fori_loop(0, pairs, attend, 0)
    others[0].wait()
    one_out[...] = wide[HALO:, :] + jnp.dot(attn[...], wo[...], preferred_element_type=jnp.float32)

    def second(rows):
        normed_two[rows, :] = layer_norm(one_out[rows, :], gains[1:2, :]).astype(jnp.bfloat16)
        two_out[rows, :] = one_out[rows, :]

    row_blocks(tokens, second)
    others[1].wait()
    others[2].wait()

    def save(c):
        return pltpu.make_async_copy(fc_buf.at[c % 2], fc_out.at[c], fc_sem.at[c % 2])

    def feed(c, carry):
        @pl.when(c >= 2)
        def _():
            save(c - 2).wait()

        inner = jnp.dot(normed_two[...], w1[c], preferred_element_type=jnp.float32)
        fc_buf[c % 2] = inner
        save(c).start()
        two_out[...] += lax.dot_general(
            gelu(inner).astype(jnp.bfloat16), w2[c], NT, preferred_element_type=jnp.float32
        )
        return carry

    lax.fori_loop(0, chunks, feed, 0)
    save(chunks - 2).wait()
    save(chunks - 1).wait()

    def third(rows):
        final = layer_norm(two_out[rows, :], gains[2:3, :]).astype(jnp.bfloat16)
        attn[rows, :] = final
        later = pl.ds(rows.start + reach, rows.size)
        picked = jnp.sum(final.astype(jnp.float32) * emb[later, :].astype(jnp.float32), axis=-1, keepdims=True)
        pick_out[rows, :] = jnp.broadcast_to(picked, (rows.size, pick_out.shape[1]))

    row_blocks(tokens, third)
    place = lax.broadcasted_iota(jnp.int32, (tokens, tokens), 0)
    rows_out[...] = jnp.dot(
        (place == rank_row[...]).astype(jnp.bfloat16), attn[...], preferred_element_type=jnp.float32
    ).astype(jnp.bfloat16)


def forward(emb, pos, seg_col, seg_row, rank_row, gains, down, up_query, up_value, weights):
    wq, wo, w1, w2 = weights
    reach, width = pos.shape
    tokens = reach - HALO
    pairs, chunks, hidden = wq.shape[0], w1.shape[0], w1.shape[2]
    f32, bf16 = jnp.float32, jnp.bfloat16
    vmem, hbm = pl.BlockSpec(memory_space=pltpu.VMEM), pl.BlockSpec(memory_space=pl.ANY)
    return pl.pallas_call(
        forward_kernel,
        out_shape=(
            jax.ShapeDtypeStruct((tokens, width), bf16),
            jax.ShapeDtypeStruct((tokens, 128), f32),
            jax.ShapeDtypeStruct((reach, width), bf16),
            jax.ShapeDtypeStruct((reach, 128), bf16),
            jax.ShapeDtypeStruct((pairs, tokens, PAIR), bf16),
            jax.ShapeDtypeStruct((pairs, reach, PAIR), bf16),
            jax.ShapeDtypeStruct((pairs, reach, PAIR), bf16),
            jax.ShapeDtypeStruct((tokens, width), f32),
            jax.ShapeDtypeStruct((tokens, width), f32),
            jax.ShapeDtypeStruct((chunks, tokens, hidden), f32),
        ),
        in_specs=[vmem] * 9 + [hbm] * 4,
        out_specs=(vmem,) * 9 + (hbm,),
        scratch_shapes=[
            pltpu.VMEM((pairs // 2, width, 6 * PAIR), bf16),
            pltpu.VMEM(wo.shape, bf16),
            pltpu.VMEM(w1.shape, bf16),
            pltpu.VMEM(w2.shape, bf16),
            pltpu.VMEM((reach, width), f32),
            pltpu.VMEM((tokens, width), bf16),
            pltpu.VMEM((tokens, width), bf16),
            pltpu.VMEM((2, tokens, hidden), f32),
            pltpu.SemaphoreType.DMA((pairs,)),
            pltpu.SemaphoreType.DMA((3,)),
            pltpu.SemaphoreType.DMA((2,)),
        ],
        compiler_params=pltpu.CompilerParams(vmem_limit_bytes=VMEM_CAP),
        name="forward",
    )(emb, pos, seg_col, seg_row, rank_row, gains, down, up_query, up_value, wq, wo, w1, w2)


def backward_kernel(
    grad_rows,
    lse_row,
    rank_col,
    pick,
    weight_col,
    target_emb,
    one,
    two,
    gains,
    seg_col,
    seg_row,
    query,
    key,
    value,
    normed,
    low,
    up_query,
    up_value,
    fc_hbm,
    wo_hbm,
    w1_hbm,
    w2_hbm,
    out,
    wo,
    w1,
    w2,
    fc_buf,
    grad_two,
    grad_low,
    grad_inner,
    grad_mixed,
    grad_query,
    grad_value,
    w_sem,
    fc_sem,
):
    tokens, width = two.shape
    pairs, chunks = query.shape[0], w1.shape[0]
    loads = [
        pltpu.make_async_copy(a, b, w_sem.at[i]) for i, (a, b) in enumerate(((w2_hbm, w2), (w1_hbm, w1), (wo_hbm, wo)))
    ]

    def fetch(c):
        return pltpu.make_async_copy(fc_hbm.at[c], fc_buf.at[c % 2], fc_sem.at[c % 2])

    loads[0].start()
    fetch(0).start()
    loads[1].start()
    loads[2].start()

    chosen = rank_col[...] == lax.broadcasted_iota(jnp.int32, (tokens, tokens), 1)
    grad_two[...] = jnp.dot(chosen.astype(jnp.bfloat16), grad_rows[...], preferred_element_type=jnp.float32)
    lse = jnp.sum(jnp.where(chosen, lse_row[...], 0.0), axis=-1, keepdims=True)
    weight = weight_col[...]
    loss = jnp.sum(weight * (lse - pick[:, 0:1]))
    grad_value[0:tokens, 0:128] = jnp.broadcast_to(jnp.exp(pick[:, 0:1] - lse) - 1.0, (tokens, 128))

    def first(rows):
        factor = grad_value[rows, 0:1]
        grad_final = weight_col[rows, :] * (grad_two[rows, :] + factor * target_emb[rows, :].astype(jnp.float32))
        grad = norm_back(two[rows, :], gains[2:3, :], grad_final)
        grad_two[rows, :] = grad
        grad_low[rows, :] = grad.astype(jnp.bfloat16)

    row_blocks(tokens, first)
    grad_inner[...] = jnp.zeros_like(grad_inner)
    for load in loads[:2]:
        load.wait()

    def feed(c, carry):
        fetch(c).wait()

        @pl.when(c + 1 < chunks)
        def _():
            fetch(c + 1).start()

        grad_act = jnp.dot(grad_low[...], w2[c], preferred_element_type=jnp.float32)
        grad_in = (grad_act * gelu_slope(fc_buf[c % 2])).astype(jnp.bfloat16)
        grad_inner[...] += lax.dot_general(grad_in, w1[c], NT, preferred_element_type=jnp.float32)
        return carry

    lax.fori_loop(0, chunks, feed, 0)

    def second(rows):
        grad_one = grad_two[rows, :] + norm_back(one[rows, :], gains[1:2, :], grad_inner[rows, :])
        grad_low[rows, :] = grad_one.astype(jnp.bfloat16)

    row_blocks(tokens, second)
    loads[2].wait()
    grad_mixed[...] = lax.dot_general(grad_low[...], wo[...], NT, preferred_element_type=jnp.float32).astype(jnp.bfloat16)
    grad_value[...] = jnp.zeros_like(grad_value)

    def attend(p, carry):
        cols = pl.ds(pl.multiple_of(p * PAIR, PAIR), PAIR)
        for block in range(tokens // PAIR):
            allowed = allowed_keys(seg_col, seg_row, block)
            rows = slice(block * PAIR, (block + 1) * PAIR)
            window = slice(block * PAIR, block * PAIR + 2 * PAIR)
            keys, values, mixed = key[p, window, :], value[p, window, :], grad_mixed[rows, cols]
            grads_q, grads_v = [], []
            for h in range(2):
                prob = probs_of(query[p, rows, :], keys, h, allowed)
                grad_prob = lax.dot_general(only_head(mixed, h), values, NT, preferred_element_type=jnp.float32)
                inner = jnp.sum(prob * grad_prob, axis=-1, keepdims=True)
                grad_score = (prob * (grad_prob - inner)).astype(jnp.bfloat16)
                grads_q.append(jnp.dot(grad_score, keys, preferred_element_type=jnp.float32) * SCORE_SCALE)
                grads_v.append(lax.dot_general(prob.astype(jnp.bfloat16), mixed, TN, preferred_element_type=jnp.float32))
            grad_query[rows, cols] = jnp.where(head_lanes(grads_q[0].shape, 0), grads_q[0], grads_q[1]).astype(
                jnp.bfloat16
            )
            grad_value[window, cols] += jnp.where(head_lanes(grads_v[0].shape, 0), grads_v[0], grads_v[1])
        return carry

    lax.fori_loop(0, pairs, attend, 0)
    grad_v = grad_value[...].astype(jnp.bfloat16)
    grad_q = grad_query[...]
    low_q = lax.dot_general(grad_q, up_query[...], NT, preferred_element_type=jnp.float32).astype(jnp.bfloat16)
    low_v = lax.dot_general(grad_v, up_value[...], NT, preferred_element_type=jnp.float32).astype(jnp.bfloat16)
    grad_down = lax.dot_general(low_q, normed[HALO:, :], TN, preferred_element_type=jnp.float32)
    grad_down += lax.dot_general(low_v, normed[...], TN, preferred_element_type=jnp.float32)
    up_q = lax.dot_general(low[HALO:, :], grad_q, TN, preferred_element_type=jnp.float32)
    up_v = lax.dot_general(low[...], grad_v, TN, preferred_element_type=jnp.float32)
    out[0:8, :] = grad_down[0:8, :]
    first_rows = lax.broadcasted_iota(jnp.int32, (8, width), 0) < 4
    out[8:16, :] = ADAPTER_SCALE * jnp.where(first_rows, up_q[0:8, :], up_v[0:8, :])
    out[16:24, :] = jnp.broadcast_to(loss, (8, width))


def backward(grad_rows, lse_row, rank_col, pick, weight_col, target_emb, saved, gains, seg_col, seg_row, up_query, up_value, weights):
    normed, low, query, key, value, one, two, fc = saved
    _, wo, w1, w2 = weights
    tokens, width = one.shape
    reach, hidden = normed.shape[0], w1.shape[2]
    f32, bf16 = jnp.float32, jnp.bfloat16
    vmem, hbm = pl.BlockSpec(memory_space=pltpu.VMEM), pl.BlockSpec(memory_space=pl.ANY)
    return pl.pallas_call(
        backward_kernel,
        out_shape=jax.ShapeDtypeStruct((24, width), f32),
        in_specs=[vmem] * 18 + [hbm] * 4,
        out_specs=vmem,
        scratch_shapes=[
            pltpu.VMEM(wo.shape, bf16),
            pltpu.VMEM(w1.shape, bf16),
            pltpu.VMEM(w2.shape, bf16),
            pltpu.VMEM((2, tokens, hidden), f32),
            pltpu.VMEM((tokens, width), f32),
            pltpu.VMEM((tokens, width), bf16),
            pltpu.VMEM((tokens, width), f32),
            pltpu.VMEM((tokens, width), bf16),
            pltpu.VMEM((tokens, width), bf16),
            pltpu.VMEM((reach, width), f32),
            pltpu.SemaphoreType.DMA((3,)),
            pltpu.SemaphoreType.DMA((2,)),
        ],
        compiler_params=pltpu.CompilerParams(vmem_limit_bytes=VMEM_CAP),
        name="backward",
    )(
        grad_rows, lse_row, rank_col, pick, weight_col, target_emb, one, two, gains, seg_col, seg_row,
        query, key, value, normed, low, up_query, up_value, fc, wo, w1, w2,
    )


def finish_kernel(
    src, master, first, second, mask, scalars, stats, new_first, new_second, new_master, new_copy,
    got, squares, squares_got, own_sem, send_sem, recv_sem, send_two, recv_two,
):
    dp, mp = lax.axis_index("dp"), lax.axis_index("mp")
    groups, copies_of = LINE * SIDE, 4
    total = groups * copies_of
    peers = [
        {"dp": lax.rem(dp + k // groups, copies_of), "mp": lax.rem(mp + k % groups, groups)} for k in range(1, total)
    ]
    greet(peers)
    copies = []
    for k in range(1, total):
        copy = remote(
            src.at[lax.rem(mp + k % groups, groups)], got.at[k], send_sem.at[k], recv_sem.at[k], peers[k - 1]
        )
        copy.start()
        copies.append(copy)
    own = pltpu.make_async_copy(src.at[mp], got.at[0], own_sem)
    own.start()
    own.wait()
    grads = got[0]
    for k in range(1, total):
        copies[k - 1].wait_recv()
    for k in range(1, total):
        grads = grads + got[k]
    loss = grads[16:24, :]
    grads = grads[0:16, :]
    squares[...] = jnp.broadcast_to(jnp.sum(grads * grads), squares.shape)
    again = []
    for k in range(1, groups):
        copy = remote(squares, squares_got.at[k], send_two.at[k], recv_two.at[k], peers[k - 1])
        copy.start()
        again.append(copy)
    for copy in again:
        copy.wait()
    square_sum = squares[...]
    for k in range(1, groups):
        square_sum = square_sum + squares_got[k]
    norm = jnp.sqrt(square_sum)
    stats[0] = loss
    stats[1] = norm
    clipped = grads * jnp.minimum(1.0, CLIP_NORM / (norm[0:1, :] + 1e-06))
    one = BETA_ONE * first[...] + (1.0 - BETA_ONE) * clipped
    two = BETA_TWO * second[...] + (1.0 - BETA_TWO) * clipped * clipped
    one_hat = one / scalars[0:1, :]
    two_hat = two / scalars[1:2, :]
    weight = master[...] - LEARN_RATE * (one_hat / (jnp.sqrt(two_hat) + ADAM_EPS) + WEIGHT_DECAY * master[...])
    keep = mask[...]
    new_first[...] = keep * one
    new_second[...] = keep * two
    new_master[...] = keep * weight
    new_copy[...] = (keep * weight).astype(jnp.bfloat16)
    for copy in copies:
        copy.wait_send()


def finish(grads, master, first, second, mask, scalars, collective):
    groups = lax.axis_size("mp")
    width = grads.shape[1]
    cols = width // groups
    slices = jnp.transpose(grads.reshape(24, groups, cols), (1, 0, 2))
    if not is_own_mesh():
        summed = lax.psum(lax.psum_scatter(slices, "mp", scatter_dimension=0), "dp")
        owned = summed[:16]
        norm = jnp.sqrt(lax.psum(jnp.sum(owned * owned), "mp"))
        clipped = owned * jnp.minimum(1.0, CLIP_NORM / (norm + 1e-06))
        one = BETA_ONE * first + (1.0 - BETA_ONE) * clipped
        two = BETA_TWO * second + (1.0 - BETA_TWO) * clipped * clipped
        weight = master - LEARN_RATE * (
            one / scalars[0, 0] / (jnp.sqrt(two / scalars[1, 0]) + ADAM_EPS) + WEIGHT_DECAY * master
        )
        kept = mask * weight
        return summed[16, 0], norm, mask * one, mask * two, kept, kept.astype(jnp.bfloat16)
    vmem = pl.BlockSpec(memory_space=pltpu.VMEM)
    tile = jax.ShapeDtypeStruct((16, cols), jnp.float32)
    total = groups * 4
    stats, one, two, weight, copy = pl.pallas_call(
        finish_kernel,
        out_shape=(jax.ShapeDtypeStruct((2, 8, cols), jnp.float32), tile, tile, tile, jax.ShapeDtypeStruct((16, cols), jnp.bfloat16)),
        in_specs=[vmem] * 6,
        out_specs=(vmem,) * 5,
        scratch_shapes=[
            pltpu.VMEM((total, 24, cols), jnp.float32),
            pltpu.VMEM((8, cols), jnp.float32),
            pltpu.VMEM((groups, 8, cols), jnp.float32),
            pltpu.SemaphoreType.DMA,
            pltpu.SemaphoreType.DMA((total,)),
            pltpu.SemaphoreType.DMA((total,)),
            pltpu.SemaphoreType.DMA((groups,)),
            pltpu.SemaphoreType.DMA((groups,)),
        ],
        compiler_params=pltpu.CompilerParams(collective_id=collective, has_side_effects=True),
        name="finish",
    )(slices, master, first, second, mask, scalars)
    return stats[0, 0, 0], stats[1, 0, 0], one, two, weight, copy


ROUND_ROWS = 80


def fetch_rows(embedding, ids, parts, tokens, collective):
    groups, mine = lax.axis_size("mp"), lax.axis_index("mp")
    vocab_local, width = embedding.shape
    seq = ids.shape[1]
    reach = HALO + tokens
    window = reach + 8
    spots = jnp.arange(parts)[:, None] * tokens - HALO + jnp.arange(window)[None, :]
    spots = jnp.clip(spots, 0, seq - 1)
    wanted = ids[:, spots].reshape(groups, window)
    holder = wanted // vocab_local
    if not is_own_mesh():
        near = wanted - mine * vocab_local
        inside = (near >= 0) & (near < vocab_local)
        rows = jnp.where(inside[..., None], jnp.take(embedding, jnp.clip(near, 0, vocab_local - 1), axis=0), 0)
        rows = lax.psum_scatter(rows, "mp", scatter_dimension=0)
        rows = jnp.concatenate([rows[:reach], rows[HALO + 1 : HALO + 1 + tokens]], axis=0)
        return jnp.float32(0.0), lambda rounds: rows
    earlier = jnp.arange(window)[:, None] > jnp.arange(window)[None, :]
    same = wanted[:, :, None] == wanted[:, None, :]
    lead = jnp.logical_not(jnp.any(same & earlier[None], axis=2))
    below = (holder[:, :, None] == holder[:, None, :]) & (wanted[:, None, :] < wanted[:, :, None]) & lead[:, None, :]
    slot = jnp.sum(below.astype(jnp.int32), axis=2)
    need = (jnp.max(slot) + 1).astype(jnp.float32)
    asked = lead & (holder == mine)
    my_slot = lax.dynamic_index_in_dim(slot, mine, 0, keepdims=False)
    my_holder = lax.dynamic_index_in_dim(holder, mine, 0, keepdims=False)

    def listed(values):
        return jnp.concatenate([values[:reach], values[HALO + 1 : HALO + 1 + tokens]])

    list_slot, list_holder = listed(my_slot), listed(my_holder)

    def one_round(r):
        base = r * ROUND_ROWS
        hit = asked[:, None, :] & (slot[:, None, :] == base + jnp.arange(ROUND_ROWS)[None, :, None])
        chosen = jnp.sum(jnp.where(hit, wanted[:, None, :] - mine * vocab_local, 0), axis=2)
        rows = jnp.take(embedding, chosen.reshape(-1), axis=0, mode="clip").reshape(groups, ROUND_ROWS, width)
        got = swap(rows, True, collective).reshape(groups * ROUND_ROWS, width)
        place = list_slot - base
        place = jnp.where((place >= 0) & (place < ROUND_ROWS), list_holder * ROUND_ROWS + place, -1)
        pick = (place[:, None] == jnp.arange(groups * ROUND_ROWS)[None, :]).astype(jnp.bfloat16)
        return jnp.dot(pick, got, preferred_element_type=jnp.float32).astype(jnp.bfloat16)

    def all_rounds(rounds):
        def lap(state):
            r, so_far = state
            return r + 1, so_far + one_round(r)

        return lax.while_loop(lambda state: state[0] < rounds, lap, (jnp.int32(1), one_round(jnp.int32(0))))[1]

    return need, all_rounds


def local(
    packed_token_rows,
    example_numbers,
    completion,
    global_token_count,
    owners,
    optimizer_step,
    embedding,
    positions,
    gains,
    query_key_value_weight,
    attention_output_weight,
    feedforward_input_weight,
    feedforward_output_weight,
    adapter_down_weight,
    adapter_up_weight,
    master,
    first_moment,
    second_moment,
):
    groups, mine = lax.axis_size("mp"), lax.axis_index("mp")
    batch, seq = packed_token_rows.shape
    width = embedding.shape[1]
    vocab_local = embedding.shape[0]
    tokens = batch * seq // groups
    parts = seq // tokens
    reach = HALO + tokens
    row, part = mine // parts, mine % parts
    start = part * tokens
    rank_size = adapter_down_weight.shape[1]
    pairs = width // PAIR
    head_cols = query_key_value_weight.shape[2]

    places = jnp.arange(seq, dtype=jnp.int32)
    is_valid = (
        (places[None, :] < seq - 1)
        & (jnp.roll(example_numbers, -1, axis=1) == example_numbers)
        & (jnp.roll(completion, -1, axis=1) == 1)
    ).reshape(groups, tokens)
    before = (jnp.arange(tokens)[:, None] < jnp.arange(tokens)[None, :]).astype(jnp.bfloat16)
    rank = jnp.dot(is_valid.astype(jnp.bfloat16), before, preferred_element_type=jnp.float32).astype(jnp.int32)
    rank = jnp.where(is_valid, rank, -1)
    targets = jnp.roll(packed_token_rows, -1, axis=1).reshape(groups, tokens)
    need_rows = jnp.max(jnp.sum(is_valid.astype(jnp.float32), axis=1))

    need_slots, all_rounds = fetch_rows(embedding, packed_token_rows, parts, tokens, 1)
    agreed = agree(jnp.stack([need_slots, need_rows]), 2)
    rounds = ((agreed[0].astype(jnp.int32) + ROUND_ROWS - 1) // ROUND_ROWS).astype(jnp.int32)
    emb = all_rounds(rounds)

    wq = query_key_value_weight.reshape(width, 3 * head_cols)
    up_rows = adapter_up_weight.reshape(2 * rank_size, head_cols)
    if is_own_mesh():
        extra = jnp.pad(up_rows, ((0, 64 - 2 * rank_size), (0, 2 * head_cols)))
        wq = jnp.concatenate([wq, extra], axis=0)
        wq, wo, w1, w2 = gather_weights(
            [wq, attention_output_weight, feedforward_input_weight, feedforward_output_weight], 3
        )
        up_all = jnp.transpose(wq[:, width : width + 2 * rank_size, :head_cols], (1, 0, 2))
    else:
        wq, wo, w1, w2, up_all = gather_weights(
            [wq, attention_output_weight, feedforward_input_weight, feedforward_output_weight, up_rows], 3
        )
        wq = jnp.transpose(wq.reshape(groups, width, 3, head_cols), (1, 2, 0, 3)).reshape(width, 3, pairs, PAIR)
        wq = jnp.transpose(wq, (2, 0, 1, 3)).reshape(pairs, width, 3 * PAIR)
        up_all = jnp.transpose(up_all, (1, 0, 2))
    wo = wo.reshape(width, width)
    weights = (wq, wo, w1, w2)
    up_all = (ADAPTER_SCALE * up_all.reshape(2 * rank_size, width).astype(jnp.float32)).astype(jnp.bfloat16)
    up_query = jnp.pad(up_all[:rank_size], ((0, 128 - rank_size), (0, 0)))
    up_value = jnp.pad(up_all[rank_size:], ((rank_size, 128 - 2 * rank_size), (0, 0)))
    down = jnp.pad(adapter_down_weight.reshape(2 * rank_size, width), ((0, 128 - 2 * rank_size), (0, 0)))

    def window_of(values):
        first = lax.dynamic_slice_in_dim(values, jnp.maximum(start - HALO, 0), HALO, 0)
        return jnp.concatenate([first, lax.dynamic_slice_in_dim(values, start, tokens, 0)], axis=0)

    pos = window_of(positions)
    seg = window_of(lax.dynamic_index_in_dim(example_numbers, row, 0, keepdims=False))
    seg = jnp.where((jnp.arange(reach) < HALO) & (part == 0), -1, seg)
    my_rank = lax.dynamic_index_in_dim(rank, mine, 0, keepdims=False)
    my_valid = (my_rank >= 0).astype(jnp.float32)
    seg_col, seg_row = seg[:, None], seg[None, :]
    rows_c, pick, normed, low, query, key, value, one, two, fc = forward(
        emb, pos, seg_col, seg_row, my_rank[None, :], gains, down, up_query, up_value, weights
    )

    def head_of(count, collective):
        def run(rows_in):
            everyone = spread(rows_in[:count], collective).reshape(groups * count, width)
            spot = rank[:, None, :] == jnp.arange(count, dtype=jnp.int32)[None, :, None]
            wanted = jnp.sum(jnp.where(spot, targets[:, None, :], 0), axis=2) - mine * vocab_local
            grad, total = head(everyone, wanted.reshape(groups * count, 1), embedding)
            total = total[:, 0].reshape(groups, count)
            if is_own_mesh():
                lanes = -(-count // 128) * 128
                totals = swap(jnp.pad(total, ((0, 0), (0, lanes - count))), False, collective + 1)[:, :, :count]
            else:
                totals = lax.all_gather(total, "mp", axis=0)
            peak = jnp.max(totals, axis=0)
            lse = peak + jnp.log(jnp.sum(jnp.exp(totals - peak[None]), axis=0))
            grad = grad.reshape(groups, count, width) * jnp.exp(total - lse)[:, :, None]
            summed = collect(grad.astype(jnp.bfloat16), collective + 2)
            my_lse = lax.dynamic_index_in_dim(lse, mine, 0, keepdims=False)
            return (
                jnp.pad(summed, ((0, tokens - count), (0, 0))),
                jnp.pad(my_lse, (0, tokens - count)),
            )

        return run

    counts = (tokens * 9 // 16, tokens * 3 // 4, tokens)
    size = (agreed[1] > counts[0]).astype(jnp.int32) + (agreed[1] > counts[1]).astype(jnp.int32)
    grad_rows, lse = lax.switch(size, [head_of(count, 4 + 3 * i) for i, count in enumerate(counts)], rows_c)

    weight_col = (my_valid / global_token_count.astype(jnp.float32))[:, None]
    grads = backward(
        grad_rows, lse[None, :], my_rank[:, None], pick, weight_col, emb[reach:],
        (normed, low, query, key, value, one, two, fc), gains, seg_col, seg_row, up_query, up_value, weights,
    )

    dp_index = lax.axis_index("dp")
    cols = master.shape[2]
    flat = (4 * rank_size, cols)
    mask = jnp.broadcast_to((owners == dp_index).astype(jnp.float32).reshape(4 * rank_size, 1), flat)
    step = optimizer_step.astype(jnp.float32)
    scalars = jnp.stack([1.0 - jnp.power(BETA_ONE, step), 1.0 - jnp.power(BETA_TWO, step)])
    scalars = jnp.broadcast_to(jnp.pad(scalars, (0, 6))[:, None], (8, cols))
    loss, norm, new_first, new_second, new_master, new_copy = finish(
        grads, master.reshape(flat), first_moment.reshape(flat), second_moment.reshape(flat), mask, scalars, 13
    )
    shape = (1,) + master.shape
    return (
        loss,
        norm,
        new_first.reshape(shape),
        new_second.reshape(shape),
        new_master.reshape(shape),
        new_copy.reshape(shape),
    )


def solution(mesh):
    return jax.shard_map(
        local,
        mesh=mesh,
        in_specs=(
            P("dp", None),
            P("dp", None),
            P("dp", None),
            P(),
            P(),
            P(),
            P("mp", None),
            P(),
            P(),
            P(None, None, "mp"),
            P("mp", None),
            P(None, "mp"),
            P(None, "mp"),
            P(),
            P(None, None, "mp"),
            P(None, None, "mp"),
            P(None, None, "mp"),
            P(None, None, "mp"),
        ),
        out_specs=(
            P(),
            P(),
            P("dp", None, None, "mp"),
            P("dp", None, None, "mp"),
            P("dp", None, None, "mp"),
            P("dp", None, None, "mp"),
        ),
        check_vma=False,
    )
```

```python
import functools

import jax
import jax.numpy as jnp
from jax import lax
from jax.experimental import pallas as pl
from jax.experimental.pallas import tpu as pltpu
from jax.sharding import PartitionSpec as P

HEAD_DIM = 64
EPS_NORM = 1e-05
ADAPTER_SCALE = 8.0
SCORE_SCALE = 0.125
MASK_VALUE = -1e30
CLIP_NORM = 1.0
BETA_ONE = 0.9
BETA_TWO = 0.999
LEARN_RATE = 0.01
WEIGHT_DECAY = 0.01
ADAM_EPS = 1e-08
HALO = 128
PAIR = 128
NT = (((1,), (1,)), ((), ()))
TN = (((0,), (0,)), ((), ()))
MESH = pl.DeviceIdType.MESH
VMEM_CAP = 62 * 2**20
LINE = 4
SIDE = 2


def is_own_mesh():
    return lax.axis_size("dp") == 4 and lax.axis_size("mp") == LINE * SIDE


def here():
    dp, mp = lax.axis_index("dp"), lax.axis_index("mp")
    return dp // 2, dp % 2, mp // SIDE, mp % SIDE


def dev(x, core, line, side):
    return {"dp": x * 2 + core, "mp": line * SIDE + side}


def greet(peers):
    barrier = pltpu.get_barrier_semaphore()
    for peer in peers:
        pl.semaphore_signal(barrier, inc=1, device_id=peer, device_id_type=MESH)
    pl.semaphore_wait(barrier, len(peers))


def greet_line(x, core, line, side, others):
    barrier = pltpu.get_barrier_semaphore()
    for peer in others:
        pl.semaphore_signal(barrier, inc=1, device_id=peer, device_id_type=MESH)

    @pl.when(line > 0)
    def _():
        pl.semaphore_signal(barrier, inc=1, device_id=dev(x, core, line - 1, side), device_id_type=MESH)

    @pl.when(line < LINE - 1)
    def _():
        pl.semaphore_signal(barrier, inc=1, device_id=dev(x, core, line + 1, side), device_id_type=MESH)

    inner = (line > 0) & (line < LINE - 1)

    @pl.when(inner)
    def _():
        pl.semaphore_wait(barrier, len(others) + 2)

    @pl.when(jnp.logical_not(inner))
    def _():
        pl.semaphore_wait(barrier, len(others) + 1)


def remote(src, dst, send_sem, recv_sem, peer):
    return pltpu.make_async_remote_copy(
        src_ref=src, dst_ref=dst, send_sem=send_sem, recv_sem=recv_sem, device_id=peer, device_id_type=MESH
    )


def swap_kernel(per_peer, src, dst, own_sem, send_sem, recv_sem):
    dp, mp = lax.axis_index("dp"), lax.axis_index("mp")
    count = LINE * SIDE
    peers = [{"dp": dp, "mp": lax.rem(mp + k, count)} for k in range(1, count)]
    greet(peers)
    copies = []
    for k in range(1, count):
        block = src.at[lax.rem(mp + k, count)] if per_peer else src
        copy = remote(block, dst.at[mp], send_sem.at[k], recv_sem.at[k], peers[k - 1])
        copy.start()
        copies.append(copy)
    own = pltpu.make_async_copy(src.at[mp] if per_peer else src, dst.at[mp], own_sem)
    own.start()
    own.wait()
    for copy in copies:
        copy.wait()


def swap(array, per_peer, collective):
    count = LINE * SIDE
    shape = array.shape if per_peer else (count,) + array.shape
    return pl.pallas_call(
        functools.partial(swap_kernel, per_peer),
        out_shape=jax.ShapeDtypeStruct(shape, array.dtype),
        in_specs=[pl.BlockSpec(memory_space=pltpu.VMEM)],
        out_specs=pl.BlockSpec(memory_space=pltpu.VMEM),
        scratch_shapes=[
            pltpu.SemaphoreType.DMA,
            pltpu.SemaphoreType.DMA((count,)),
            pltpu.SemaphoreType.DMA((count,)),
        ],
        compiler_params=pltpu.CompilerParams(
            collective_id=collective, has_side_effects=True, vmem_limit_bytes=VMEM_CAP
        ),
        name=f"swap_{collective}",
    )(array)


def agree_kernel(src, out, got, send_sem, recv_sem):
    dp, mp = lax.axis_index("dp"), lax.axis_index("mp")
    peers = [{"dp": lax.rem(dp + k, 4), "mp": mp} for k in range(1, 4)]
    greet(peers)
    copies = []
    for k in range(1, 4):
        copy = remote(src, got.at[k - 1], send_sem.at[k - 1], recv_sem.at[k - 1], peers[k - 1])
        copy.start()
        copies.append(copy)
    for copy in copies:
        copy.wait()
    out[...] = jnp.maximum(jnp.maximum(src[...], got[0]), jnp.maximum(got[1], got[2]))


def agree(values, collective):
    if not is_own_mesh():
        return lax.pmax(values, "dp")
    tile = jnp.zeros((8, 128), jnp.float32).at[0, : values.shape[0]].set(values)
    out = pl.pallas_call(
        agree_kernel,
        out_shape=jax.ShapeDtypeStruct((8, 128), jnp.float32),
        in_specs=[pl.BlockSpec(memory_space=pltpu.VMEM)],
        out_specs=pl.BlockSpec(memory_space=pltpu.VMEM),
        scratch_shapes=[
            pltpu.VMEM((3, 8, 128), jnp.float32),
            pltpu.SemaphoreType.DMA((3,)),
            pltpu.SemaphoreType.DMA((3,)),
        ],
        compiler_params=pltpu.CompilerParams(collective_id=collective, has_side_effects=True),
        name="agree",
    )(tile)
    return out[0, : values.shape[0]]


def weight_events(sizes):
    events, start = [], 0.0
    for k, size in enumerate(sizes):
        events.append((start - 1.5 * size - 0.001 if k else -1.0, "own", k, 0))
        for step in range(LINE):
            arrive = start + size * min(step, 2.5)
            if step:
                events.append((arrive, "line", k, step))
            events.append((arrive + 0.6 * size, "side", k, step))
            events.append((arrive + 1.2 * size, "x", k, step))
        start += 2.5 * size
    return sorted(events)


def weight_kernel(sizes, *refs):
    n = len(sizes)
    src, own_vmem, full = refs[:n], refs[n : 2 * n], refs[2 * n : 3 * n]
    own_sem = refs[3 * n]
    line_s, line_r, side_s, side_r, x_s, x_r, xf_s, xf_r, sib_s, sib_r, sib2_s, sib2_r, sib3_s, sib3_r = refs[3 * n + 1 :]
    x, core, line, side = here()
    up, down = dev(x, core, line + 1, side), dev(x, core, line - 1, side)
    across, twin, sibling = dev(x, core, line, 1 - side), dev(1 - x, core, line, side), dev(x, 1 - core, line, side)
    greet_line(x, core, line, side, [across, twin, sibling])
    mine = line * SIDE + side

    def piece(k, block, c, h):
        rows = full[k].shape[1]
        if h is None:
            return full[k].at[block, pl.ds(c * (rows // 2), rows // 2)]
        return full[k].at[block, pl.ds((c * 2 + h) * (rows // 4), rows // 4)]

    def own_piece(k, c, h):
        rows = full[k].shape[1]
        if h is None:
            return src[k].at[pl.ds(c * (rows // 2), rows // 2)]
        return src[k].at[pl.ds((c * 2 + h) * (rows // 4), rows // 4)]

    pending = []

    def when(cond, action):
        if cond is None:
            action()
        else:
            pl.when(cond)(action)

    def send(cond, src_ref, dst_ref, ssem, rsem, peer):
        copy = remote(src_ref, dst_ref, ssem, rsem, peer)
        when(cond, copy.start)
        pending.append((cond, copy))

    def arrived(cond, dst_ref, ssem, rsem):
        when(cond, remote(dst_ref, dst_ref, ssem, rsem, across).wait_recv)

    def exists(direction, step):
        if step == 0:
            return None
        return line >= step if direction == 0 else line + step < LINE

    def block_line(direction, step):
        return line - step if direction == 0 else line + step

    def flows(step):
        return (0,) if step == 0 else (0, 1)

    def both(first, second):
        return second if first is None else (first if second is None else first & second)

    def pass_on(k, step):
        for direction in flows(step):
            cond = exists(direction, step)
            block = block_line(direction, step) * SIDE + side
            far = step == LINE - 1
            whole = own_piece(k, core, None) if step == 0 else piece(k, block, core, None)
            part = own_piece(k, core, x) if step == 0 else piece(k, block, core, x)
            for way in (0, 1) if step == 0 else (direction,):
                if step < LINE - 1:
                    ok = both(cond, line < LINE - 1 if way == 0 else line > 0)
                    last = step + 1 == LINE - 1
                    send(
                        ok,
                        part if last else whole,
                        piece(k, block, core, x if last else None),
                        line_s.at[k, way, step],
                        line_r.at[k, way, step],
                        up if way == 0 else down,
                    )
            send(cond, part, piece(k, block, core, x), side_s.at[k, direction, step], side_r.at[k, direction, step], across)
            if far:
                send(cond, part, piece(k, block, core, x), xf_s.at[k, direction], xf_r.at[k, direction], twin)
            if step:
                send(
                    cond,
                    part if far else whole,
                    piece(k, block, core, x if far else None),
                    sib_s.at[k, direction, step],
                    sib_r.at[k, direction, step],
                    sibling,
                )

    for k in range(n):
        pltpu.make_async_copy(own_vmem[k], full[k].at[mine], own_sem.at[k]).start()

    for _, kind, k, step in weight_events(sizes):
        if kind == "own":
            pass_on(k, 0)
            continue
        for direction in flows(step):
            cond = exists(direction, step)
            near = block_line(direction, step) * SIDE + side
            other = block_line(direction, step) * SIDE + 1 - side
            far = step == LINE - 1
            if kind == "line":
                arrived(
                    cond,
                    piece(k, near, core, x if far else None),
                    line_s.at[k, direction, step - 1],
                    line_r.at[k, direction, step - 1],
                )
            elif kind == "side":
                part = piece(k, other, core, x)
                arrived(cond, part, side_s.at[k, direction, step], side_r.at[k, direction, step])
                send(cond, part, part, x_s.at[k, direction, step], x_r.at[k, direction, step], twin)
                send(cond, part, part, sib2_s.at[k, direction, step], sib2_r.at[k, direction, step], sibling)
            else:
                part = piece(k, other, core, 1 - x)
                arrived(cond, part, x_s.at[k, direction, step], x_r.at[k, direction, step])
                send(cond, part, part, sib3_s.at[k, direction, step], sib3_r.at[k, direction, step], sibling)
                if far:
                    part = piece(k, near, core, 1 - x)
                    arrived(cond, part, xf_s.at[k, direction], xf_r.at[k, direction])
                    send(cond, part, part, sib_s.at[k, direction, 0], sib_r.at[k, direction, 0], sibling)
        if kind == "line":
            pass_on(k, step)

    other_core = 1 - core
    for k in range(n):
        for step in range(LINE):
            for direction in flows(step):
                cond = exists(direction, step)
                near = block_line(direction, step) * SIDE + side
                other = block_line(direction, step) * SIDE + 1 - side
                far = step == LINE - 1
                if step:
                    arrived(
                        cond,
                        piece(k, near, other_core, x if far else None),
                        sib_s.at[k, direction, step],
                        sib_r.at[k, direction, step],
                    )
                if far:
                    arrived(cond, piece(k, near, other_core, 1 - x), sib_s.at[k, direction, 0], sib_r.at[k, direction, 0])
                arrived(cond, piece(k, other, other_core, x), sib2_s.at[k, direction, step], sib2_r.at[k, direction, step])
                arrived(cond, piece(k, other, other_core, 1 - x), sib3_s.at[k, direction, step], sib3_r.at[k, direction, step])
    for cond, copy in pending:
        when(cond, copy.wait_send)
    for k in range(n):
        pltpu.make_async_copy(own_vmem[k], full[k].at[mine], own_sem.at[k]).wait()


def gather_weights(blocks, collective):
    if not is_own_mesh():
        return [lax.all_gather(block, "mp", axis=0) for block in blocks]
    n = len(blocks)
    total = sum(block.size for block in blocks)
    sizes = [block.size / total for block in blocks]
    grid = pltpu.SemaphoreType.DMA((n, 2, LINE))
    pair = pltpu.SemaphoreType.DMA((n, 2))
    return pl.pallas_call(
        functools.partial(weight_kernel, sizes),
        out_shape=[jax.ShapeDtypeStruct((LINE * SIDE,) + block.shape, block.dtype) for block in blocks],
        in_specs=[pl.BlockSpec(memory_space=pl.ANY)] * n + [pl.BlockSpec(memory_space=pltpu.VMEM)] * n,
        out_specs=[pl.BlockSpec(memory_space=pl.ANY)] * n,
        scratch_shapes=[pltpu.SemaphoreType.DMA((n,)), grid, grid, grid, grid, grid, grid, pair, pair]
        + [grid] * 6,
        compiler_params=pltpu.CompilerParams(
            collective_id=collective, has_side_effects=True, vmem_limit_bytes=VMEM_CAP
        ),
        name="gather_weights",
    )(*blocks, *blocks)


def spread_kernel(own, out, own_sem, line_s, line_r, side_s, side_r):
    x, core, line, side = here()
    across = dev(x, core, line, 1 - side)
    greet_line(x, core, line, side, [across])
    up, down = dev(x, core, line + 1, side), dev(x, core, line - 1, side)
    mine = line * SIDE + side
    local = pltpu.make_async_copy(own, out.at[mine], own_sem)
    local.start()
    pending = []

    def send(cond, src, block, ssem, rsem, peer):
        copy = remote(src, out.at[block], ssem, rsem, peer)
        if cond is None:
            copy.start()
        else:
            pl.when(cond)(copy.start)
        pending.append((cond, copy))

    send(line < LINE - 1, own, mine, line_s.at[0, 0], line_r.at[0, 0], up)
    send(line > 0, own, mine, line_s.at[1, 0], line_r.at[1, 0], down)
    send(None, own, mine, side_s.at[0, 0], side_r.at[0, 0], across)
    for step in range(1, LINE):
        for way in (0, 1):
            cond = line >= step if way == 0 else line + step < LINE
            block = (line - step if way == 0 else line + step) * SIDE + side
            pl.when(cond)(
                remote(out.at[block], out.at[block], line_s.at[way, step - 1], line_r.at[way, step - 1], across).wait_recv
            )
            if step < LINE - 1:
                more = cond & (line < LINE - 1 if way == 0 else line > 0)
                send(more, out.at[block], block, line_s.at[way, step], line_r.at[way, step], up if way == 0 else down)
            send(cond, out.at[block], block, side_s.at[way, step], side_r.at[way, step], across)
    for step in range(LINE):
        for way in (0,) if step == 0 else (0, 1):
            cond = line >= step if way == 0 else line + step < LINE
            block = (line - step if way == 0 else line + step) * SIDE + 1 - side
            pl.when(cond)(
                remote(out.at[block], out.at[block], side_s.at[way, step], side_r.at[way, step], across).wait_recv
            )
    for cond, copy in pending:
        if cond is None:
            copy.wait_send()
        else:
            pl.when(cond)(copy.wait_send)
    local.wait()


def spread(rows, collective):
    if not is_own_mesh():
        return lax.all_gather(rows, "mp", axis=0)
    sems = pltpu.SemaphoreType.DMA((2, LINE))
    return pl.pallas_call(
        spread_kernel,
        out_shape=jax.ShapeDtypeStruct((LINE * SIDE,) + rows.shape, rows.dtype),
        in_specs=[pl.BlockSpec(memory_space=pltpu.VMEM)],
        out_specs=pl.BlockSpec(memory_space=pl.ANY),
        scratch_shapes=[pltpu.SemaphoreType.DMA, sems, sems, sems, sems],
        compiler_params=pltpu.CompilerParams(
            collective_id=collective, has_side_effects=True, vmem_limit_bytes=VMEM_CAP
        ),
        name=f"spread_{collective}",
    )(rows)


def collect_order(line, step):
    mirror = line // 2
    near = line * (1 - mirror) + (LINE - 1 - line) * mirror
    place = (LINE - 1, LINE - 2, 1 - near, near)[step]
    return place * (1 - mirror) + (LINE - 1 - place) * mirror


def collect_kernel(src, out, side_got, line_out, line_got, side_s, side_r, line_s, line_r):
    x, core, line, side = here()
    across = dev(x, core, line, 1 - side)
    greet_line(x, core, line, side, [across])
    up, down = dev(x, core, line + 1, side), dev(x, core, line - 1, side)
    copies = []
    for step in range(LINE):
        dest = collect_order(line, step)
        copy = remote(
            src.at[dest * SIDE + 1 - side], side_got.at[step], side_s.at[step], side_r.at[step], across
        )
        copy.start()
        copies.append(copy)

    def add(target, more):
        target[...] = (target[...].astype(jnp.float32) + more[...].astype(jnp.float32)).astype(target.dtype)

    for step in range(LINE):
        dest = collect_order(line, step)
        copies[step].wait_recv()
        partial = line_out.at[step]
        partial[...] = (
            src[dest * SIDE + side].astype(jnp.float32) + side_got[step].astype(jnp.float32)
        ).astype(partial.dtype)
        for way in (0, 1):
            behind = line > 0 if way == 0 else line < LINE - 1
            onward = dest >= line if way == 0 else dest <= line

            @pl.when(behind & onward)
            def _():
                got = line_got.at[way, dest]
                remote(got, got, line_s.at[way, step], line_r.at[way, dest], across).wait_recv()
                add(partial, got)

        for way in (0, 1):
            onward = dest > line if way == 0 else dest < line

            @pl.when(onward)
            def _():
                remote(
                    partial, line_got.at[way, dest], line_s.at[way, step], line_r.at[way, dest], up if way == 0 else down
                ).start()

    out[...] = line_out[LINE - 1]
    for step in range(LINE):
        dest = collect_order(line, step)
        copies[step].wait_send()
        for way in (0, 1):

            @pl.when(dest > line if way == 0 else dest < line)
            def _():
                remote(
                    line_out.at[step], line_got.at[way, dest], line_s.at[way, step], line_r.at[way, dest], across
                ).wait_send()


def collect(parts, collective):
    if not is_own_mesh():
        return lax.psum_scatter(parts, "mp", scatter_dimension=0)
    shape = parts.shape[1:]
    sems = pltpu.SemaphoreType.DMA((LINE,))
    pairs = pltpu.SemaphoreType.DMA((2, LINE))
    return pl.pallas_call(
        collect_kernel,
        out_shape=jax.ShapeDtypeStruct(shape, parts.dtype),
        in_specs=[pl.BlockSpec(memory_space=pltpu.VMEM)],
        out_specs=pl.BlockSpec(memory_space=pltpu.VMEM),
        scratch_shapes=[
            pltpu.VMEM((LINE,) + shape, parts.dtype),
            pltpu.VMEM((LINE,) + shape, parts.dtype),
            pltpu.VMEM((2, LINE) + shape, parts.dtype),
            sems,
            sems,
            pairs,
            pairs,
        ],
        compiler_params=pltpu.CompilerParams(
            collective_id=collective, has_side_effects=True, vmem_limit_bytes=VMEM_CAP
        ),
        name=f"collect_{collective}",
    )(parts)


def head_kernel(tile, tiles, x_ref, target_ref, table_ref, grad_ref, total_ref, logit_scr, acc):
    rows = x_ref.shape[0]
    target = target_ref[...]

    def table_rows(t):
        return table_ref[pl.ds(pl.multiple_of(t * tile, tile), tile), :]

    def logits(t):
        return lax.dot_general(x_ref[...], table_rows(t), NT, preferred_element_type=jnp.float32)

    logit_scr[0] = logits(0)
    acc[...] = jnp.zeros_like(acc)

    def lap(t, carry):
        peak, total = carry
        slot = t % 2

        @pl.when(t + 1 < tiles)
        def _():
            logit_scr[1 - slot] = logits(t + 1)

        scores = logit_scr[slot]
        new_peak = jnp.maximum(peak, jnp.max(scores, axis=-1, keepdims=True))
        prob = jnp.exp(scores - new_peak)
        shrink = jnp.exp(peak - new_peak)
        total = total * shrink + jnp.sum(prob, axis=-1, keepdims=True)
        column = lax.broadcasted_iota(jnp.int32, scores.shape, 1) + t * tile
        others = jnp.where(column == target, 0.0, prob).astype(jnp.bfloat16)
        acc[...] = acc[...] * shrink + jnp.dot(others, table_rows(t), preferred_element_type=jnp.float32)
        return new_peak, total

    start = (jnp.full((rows, 1), MASK_VALUE, jnp.float32), jnp.zeros((rows, 1), jnp.float32))
    peak, total = lax.fori_loop(0, tiles, lap, start)
    grad_ref[...] = acc[...] / total
    total_ref[...] = jnp.broadcast_to(peak + jnp.log(total), total_ref.shape)


def largest_block(extent, choices):
    for choice in choices:
        if extent % choice == 0:
            return choice
    return extent


def head(rows_in, target, table):
    count, width = rows_in.shape
    vocab = table.shape[0]
    tile = largest_block(vocab, (1280, 640, 256, 128))
    rows = largest_block(count, (384, 512, 256, 128))
    return pl.pallas_call(
        functools.partial(head_kernel, tile, vocab // tile),
        out_shape=(
            jax.ShapeDtypeStruct((count, width), jnp.float32),
            jax.ShapeDtypeStruct((count, 128), jnp.float32),
        ),
        grid=(count // rows,),
        in_specs=[
            pl.BlockSpec((rows, width), lambda i: (i, 0)),
            pl.BlockSpec((rows, 1), lambda i: (i, 0)),
            pl.BlockSpec((vocab, width), lambda i: (0, 0), pipeline_mode=pl.Buffered(1)),
        ],
        out_specs=(
            pl.BlockSpec((rows, width), lambda i: (i, 0)),
            pl.BlockSpec((rows, 128), lambda i: (i, 0)),
        ),
        scratch_shapes=[pltpu.VMEM((2, rows, tile), jnp.float32), pltpu.VMEM((rows, width), jnp.float32)],
        compiler_params=pltpu.CompilerParams(vmem_limit_bytes=VMEM_CAP),
        name=f"head_{count}",
    )(rows_in, target, table)


def head_order(line, step):
    mirror = line // 2
    near = line * (1 - mirror) + (LINE - 1 - line) * mirror
    place = (near, 2, 3, 1 - near)[step]
    return place * (1 - mirror) + (LINE - 1 - place) * mirror


def traced_order(line, step):
    places = [head_order(line, k) for k in range(LINE)]
    out = places[LINE - 1]
    for k in range(LINE - 2, -1, -1):
        out = jnp.where(step == k, places[k], out)
    return out


def head_all_kernel(
    tile, tiles, own, target_ref, table_hbm, out, lse_out,
    table, got, logit_scr, acc, theirs, mine, side_got, line_got,
    st_theirs, st_mine, st_side, st_line, col_a, col_b, column,
    own_sem, table_sem, line_s, line_r, side_s, side_r,
    back_s, back_r, backst_s, backst_r, flow_s, flow_r, flowst_s, flowst_r,
):
    rows = own.shape[0]
    lanes = st_mine.shape[2]
    x, core, line, side = here()
    across = dev(x, core, line, 1 - side)
    up, down = dev(x, core, line + 1, side), dev(x, core, line - 1, side)
    table_loads = [
        pltpu.make_async_copy(table_hbm.at[pl.ds(t * tile, tile)], table.at[pl.ds(t * tile, tile)], table_sem.at[t])
        for t in range(tiles)
    ]
    for load in table_loads:
        load.start()
    local_copy = pltpu.make_async_copy(own, got.at[line * SIDE + side], own_sem)
    local_copy.start()
    greet_line(x, core, line, side, [across])
    def when(cond, action):
        if cond is None:
            action()
        else:
            pl.when(cond)(action)

    me = line * SIDE + side

    def reach_of(way, step):
        return line >= step if way == 0 else line + step < LINE

    def place_of(way, step):
        return line - step if way == 0 else line + step

    def rows_out(way, step):
        block = place_of(way, step) * SIDE + side
        src = own if step == 0 else got.at[block]
        ends = line < LINE - 1 if way == 0 else line > 0
        cond = reach_of(way, step) if step else None
        found = []
        if step < LINE - 1:
            along = remote(src, got.at[block], line_s.at[way, step], line_r.at[way, step], up if way == 0 else down)
            found.append((ends if cond is None else cond & ends, along))
        if step or way == 0:
            found.append((cond, remote(src, got.at[block], side_s.at[way, step], side_r.at[way, step], across)))
        return found

    for way in (0, 1):
        for cond, copy in rows_out(way, 0):
            when(cond, copy.start)

    def rows_event(step):
        for way in (0, 1):
            block = place_of(way, step) * SIDE + side
            arrived = remote(got.at[block], got.at[block], line_s.at[way, step - 1], line_r.at[way, step - 1], across)
            when(reach_of(way, step), arrived.wait_recv)
            for cond, copy in rows_out(way, step):
                when(cond, copy.start)

    def side_event(order_step):
        dest = head_order(line, order_step)
        for step in range(LINE):
            for way in (0,) if step == 0 else (0, 1):
                if step == 0 and order_step:
                    continue
                if step and not order_step:
                    continue
                cond = None if step == 0 else (dest == place_of(way, step))
                block = place_of(way, step) * SIDE + 1 - side
                when(cond, remote(got.at[block], got.at[block], side_s.at[way, step], side_r.at[way, step], across).wait_recv)

    def back_copies(step):
        return (
            remote(theirs.at[step], side_got.at[step], back_s.at[step], back_r.at[step], across),
            remote(st_theirs.at[step], st_side.at[step], backst_s.at[step], backst_r.at[step], across),
        )

    def flow_copies(step, way, dest):
        peer = up if way == 0 else down
        return (
            remote(mine.at[step], line_got.at[way, dest], flow_s.at[way, step], flow_r.at[way, dest], peer),
            remote(st_mine.at[step], st_line.at[way, dest], flowst_s.at[way, step], flowst_r.at[way, dest], peer),
        )

    def merge(step, more, more_st):
        a, b = st_mine[step], more_st[...]
        peak = jnp.maximum(a, b)
        ea, eb = jnp.exp(a - peak), jnp.exp(b - peak)
        total = ea + eb
        col_a[...] = jnp.transpose(jnp.broadcast_to((ea / total)[0:1], (128, lanes)))
        col_b[...] = jnp.transpose(jnp.broadcast_to((eb / total)[0:1], (128, lanes)))
        st_mine[step] = peak + jnp.log(total)
        block = largest_block(rows, (96, 64, 32, 16))

        def lap(r, carry):
            s = pl.ds(pl.multiple_of(r * block, block), block)
            joined = mine[step, s, :].astype(jnp.float32) * col_a[s, 0:1] + more[s, :].astype(jnp.float32) * col_b[s, 0:1]
            mine[step, s, :] = joined.astype(jnp.bfloat16)
            return carry

        lax.fori_loop(0, rows // block, lap, 0)

    def back_event(step):
        for copy in back_copies(step):
            copy.wait_recv()
        merge(step, side_got.at[step], st_side.at[step])

    def flow_event(step):
        dest = head_order(line, step)
        for way in (0, 1):
            behind = line > 0 if way == 0 else line < LINE - 1
            onward = dest >= line if way == 0 else dest <= line

            @pl.when(behind & onward)
            def _():
                for copy in flow_copies(step, way, dest):
                    copy.wait_recv()
                merge(step, line_got.at[way, dest], st_line.at[way, dest])

        if step:
            for way in (0, 1):

                @pl.when(dest > line if way == 0 else dest < line)
                def _():
                    for copy in flow_copies(step, way, dest):
                        copy.start()

    def table_rows(t):
        return table[pl.ds(pl.multiple_of(t * tile, tile), tile), :]

    def spot(g):
        i = g // tiles
        step = i // 2
        other = jnp.where(step == LINE - 1, 1 - i % 2, i % 2)
        which = jnp.where(other == 1, 1 - side, side)
        return step, other, traced_order(line, step) * SIDE + which

    laps = 2 * LINE * tiles

    def logits(g):
        _, _, block = spot(g)
        return lax.dot_general(got[block], table_rows(g % tiles), NT, preferred_element_type=jnp.float32)

    local_copy.wait()
    acc[...] = jnp.zeros_like(acc)
    column[...] = jnp.zeros_like(column)
    table_loads[0].wait()
    logit_scr[0] = logits(jnp.int32(0))

    events = {}

    def at(g, action, *given):
        events.setdefault(g, []).append((action, given))

    for t in range(1, tiles):
        at(t - 1, lambda t=t: table_loads[t].wait())
    edge = (line == 0) | (line == LINE - 1)

    def start_back(step):
        for copy in back_copies(step):
            copy.start()

    def flow_at(condition, step):
        pl.when(condition)(functools.partial(flow_event, step))

    inner = jnp.logical_not(edge)
    at(tiles - 1, side_event, 0)
    at(tiles, rows_event, 1)
    at(2 * tiles - 1, rows_event, 2)
    at(3 * tiles - 1, side_event, 1)
    at(3 * tiles, rows_event, 3)
    at(4 * tiles, start_back, 1)
    at(5 * tiles - 1, side_event, 2)
    at(6 * tiles - 1, side_event, 3)
    at(6 * tiles, start_back, 2)
    at(6 * tiles + 1, back_event, 1)
    at(6 * tiles + 1, flow_at, edge, 1)
    at(7 * tiles, start_back, 3)
    at(7 * tiles, start_back, 0)
    at(8 * tiles - 3, back_event, 2)
    at(8 * tiles - 3, flow_at, edge, 2)
    at(8 * tiles - 2, flow_at, inner, 1)

    def lap(g, carry):
        peak, total = carry
        for when_g, actions in sorted(events.items()):

            @pl.when(g == when_g)
            def _():
                for action, given in actions:
                    action(*given)

        t = g % tiles
        step, other, block = spot(g)
        slot = g % 2
        peak = jnp.where(t == 0, MASK_VALUE, peak)
        scores = logit_scr[slot]
        ahead = jnp.minimum(g + 1, laps - 1)
        logit_scr[1 - slot] = logits(ahead)
        new_peak = jnp.maximum(peak, jnp.max(scores, axis=-1, keepdims=True))
        prob = jnp.exp(scores - new_peak)
        shrink = jnp.exp(peak - new_peak)
        total = total * shrink + jnp.sum(prob, axis=-1, keepdims=True)
        place = lax.broadcasted_iota(jnp.int32, scores.shape, 1) + t * tile
        others = jnp.where(place == target_ref[block], 0.0, prob).astype(jnp.bfloat16)
        acc[...] = acc[...] * shrink + jnp.dot(others, table_rows(t), preferred_element_type=jnp.float32)

        @pl.when(t == tiles - 1)
        def _():
            averaged = (acc[...] / total).astype(jnp.bfloat16)
            column[0:rows, :] = jnp.broadcast_to(new_peak + jnp.log(total), (rows, 128))
            flat = jnp.transpose(column[...])[0:8]

            @pl.when(other == 1)
            def _():
                theirs[step] = averaged
                st_theirs[step] = flat

            @pl.when(other == 0)
            def _():
                mine[step] = averaged
                st_mine[step] = flat

        return new_peak, total

    start = (jnp.full((rows, 1), MASK_VALUE, jnp.float32), jnp.zeros((rows, 1), jnp.float32))
    lax.fori_loop(0, laps, lap, start)
    back_event(3)
    flow_at(edge, 3)
    flow_at(inner, 2)
    back_event(0)
    flow_at(inner, 3)
    flow_event(0)
    out[...] = mine[0]
    lse_out[...] = st_mine[0]
    for step in range(LINE):
        for way in (0, 1):
            for cond, copy in rows_out(way, step):
                when(cond, copy.wait_send)
    for step in range(LINE):
        for copy in back_copies(step):
            copy.wait_send()
        if step:
            dest = head_order(line, step)
            for way in (0, 1):

                @pl.when(dest > line if way == 0 else dest < line)
                def _():
                    for copy in flow_copies(step, way, dest):
                        copy.wait_send()


def head_all(rows_in, target, table, collective):
    rows, width = rows_in.shape
    vocab = table.shape[0]
    tile = largest_block(vocab, (1280, 640, 256, 128))
    tiles = vocab // tile
    lanes = -(-rows // 128) * 128
    bf16, f32 = jnp.bfloat16, jnp.float32
    dma = pltpu.SemaphoreType.DMA
    groups = LINE * SIDE
    return pl.pallas_call(
        functools.partial(head_all_kernel, tile, tiles),
        out_shape=(jax.ShapeDtypeStruct((rows, width), bf16), jax.ShapeDtypeStruct((8, lanes), f32)),
        in_specs=[
            pl.BlockSpec(memory_space=pltpu.VMEM),
            pl.BlockSpec(memory_space=pltpu.VMEM),
            pl.BlockSpec(memory_space=pl.ANY),
        ],
        out_specs=(pl.BlockSpec(memory_space=pltpu.VMEM), pl.BlockSpec(memory_space=pltpu.VMEM)),
        scratch_shapes=[
            pltpu.VMEM((vocab, width), bf16),
            pltpu.VMEM((groups, rows, width), bf16),
            pltpu.VMEM((2, rows, tile), f32),
            pltpu.VMEM((rows, width), f32),
            pltpu.VMEM((LINE, rows, width), bf16),
            pltpu.VMEM((LINE, rows, width), bf16),
            pltpu.VMEM((LINE, rows, width), bf16),
            pltpu.VMEM((2, LINE, rows, width), bf16),
            pltpu.VMEM((LINE, 8, lanes), f32),
            pltpu.VMEM((LINE, 8, lanes), f32),
            pltpu.VMEM((LINE, 8, lanes), f32),
            pltpu.VMEM((2, LINE, 8, lanes), f32),
            pltpu.VMEM((lanes, 128), f32),
            pltpu.VMEM((lanes, 128), f32),
            pltpu.VMEM((lanes, 128), f32),
            dma,
            dma((tiles,)),
            dma((2, LINE)),
            dma((2, LINE)),
            dma((2, LINE)),
            dma((2, LINE)),
            dma((LINE,)),
            dma((LINE,)),
            dma((LINE,)),
            dma((LINE,)),
            dma((2, LINE)),
            dma((2, LINE)),
            dma((2, LINE)),
            dma((2, LINE)),
        ],
        compiler_params=pltpu.CompilerParams(
            collective_id=collective, has_side_effects=True, vmem_limit_bytes=VMEM_CAP
        ),
        name="head_all",
    )(rows_in, target, table)


def norm_parts(values):
    center = values - jnp.mean(values, axis=-1, keepdims=True)
    spread_of = jnp.mean(center * center, axis=-1, keepdims=True)
    scale = lax.rsqrt(spread_of + EPS_NORM)
    return center * scale, scale


def layer_norm(values, gain_row):
    return norm_parts(values)[0] * gain_row


def norm_back(values, gain_row, grad_out):
    hat, scale = norm_parts(values)
    inner = grad_out * gain_row
    return scale * (
        inner
        - jnp.mean(inner, axis=-1, keepdims=True)
        - hat * jnp.mean(inner * hat, axis=-1, keepdims=True)
    )


GELU_A = 0.7978845608028654
GELU_B = 0.044715


def gelu(z):
    return 0.5 * z * (1.0 + jnp.tanh(GELU_A * (z + GELU_B * z * z * z)))


def gelu_slope(z):
    square = z * z
    curve = jnp.tanh(GELU_A * z * (1.0 + GELU_B * square))
    return 0.5 * (1.0 + curve) + 0.5 * z * (1.0 - curve * curve) * GELU_A * (1.0 + 3.0 * GELU_B * square)


def row_blocks(count, body, block=128):
    def lap(i, carry):
        body(pl.ds(pl.multiple_of(i * block, block), block))
        return carry

    lax.fori_loop(0, count // block, lap, 0)


def allowed_keys(seg_col, seg_row, block):
    rows = seg_col[HALO + block * PAIR : HALO + (block + 1) * PAIR, :]
    keys = seg_row[:, block * PAIR : block * PAIR + 2 * PAIR]
    shape = (PAIR, 2 * PAIR)
    causal = lax.broadcasted_iota(jnp.int32, shape, 1) <= lax.broadcasted_iota(jnp.int32, shape, 0) + HALO
    return causal & (rows == keys)


def head_lanes(shape, which):
    lane = lax.broadcasted_iota(jnp.int32, shape, 1)
    return lane < HEAD_DIM if which == 0 else lane >= HEAD_DIM


def only_head(values, which):
    return jnp.where(head_lanes(values.shape, which), values, jnp.zeros_like(values))


def probs_of(query, keys, which, allowed):
    scores = lax.dot_general(only_head(query, which), keys, NT, preferred_element_type=jnp.float32) * SCORE_SCALE
    scores = jnp.where(allowed, scores, MASK_VALUE)
    exp_blk = jnp.exp(scores - jnp.max(scores, axis=-1, keepdims=True))
    return exp_blk / jnp.sum(exp_blk, axis=-1, keepdims=True)


def forward_kernel(
    emb,
    pos,
    seg_col,
    seg_row,
    rank_row,
    gains,
    down,
    up_query,
    up_value,
    wq_hbm,
    wo_hbm,
    w1_hbm,
    w2_hbm,
    rows_out,
    pick_out,
    normed_out,
    low_out,
    query_out,
    key_out,
    value_out,
    one_out,
    two_out,
    fc_out,
    wq,
    wo,
    w1,
    w2,
    wide,
    attn,
    normed_two,
    fc_buf,
    wq_sem,
    w_sem,
    fc_sem,
):
    tokens = two_out.shape[0]
    reach = HALO + tokens
    pairs = query_out.shape[0]
    chunks = w1.shape[0]
    loads = []
    for p in range(pairs):
        loads.append(
            pltpu.make_async_copy(
                wq_hbm.at[p, pl.ds(0, wq.shape[1])], wq.at[p // 2, :, pl.ds((p % 2) * 3 * PAIR, 3 * PAIR)], wq_sem.at[p]
            )
        )
    others = [
        pltpu.make_async_copy(a, b, w_sem.at[i]) for i, (a, b) in enumerate(((wo_hbm, wo), (w1_hbm, w1), (w2_hbm, w2)))
    ]
    for load in loads + others:
        load.start()

    def first(rows):
        x_zero = emb[rows, :].astype(jnp.float32) + pos[rows, :].astype(jnp.float32)
        wide[rows, :] = x_zero
        normed_out[rows, :] = layer_norm(x_zero, gains[0:1, :]).astype(jnp.bfloat16)

    row_blocks(reach, first)
    low_out[...] = lax.dot_general(normed_out[...], down[...], NT, preferred_element_type=jnp.float32).astype(
        jnp.bfloat16
    )
    for load in loads:
        load.wait()

    def project(j, carry):
        both = jnp.dot(normed_out[...], wq[j], preferred_element_type=jnp.float32)
        for half in range(2):
            p = 2 * j + half
            cols = pl.ds(pl.multiple_of(p * PAIR, PAIR), PAIR)
            base = half * 3 * PAIR
            term_q = jnp.dot(low_out[HALO:, :], up_query[:, cols], preferred_element_type=jnp.float32)
            term_v = jnp.dot(low_out[...], up_value[:, cols], preferred_element_type=jnp.float32)
            query_out[p] = (both[HALO:, base : base + PAIR] + term_q).astype(jnp.bfloat16)
            key_out[p] = both[:, base + PAIR : base + 2 * PAIR].astype(jnp.bfloat16)
            value_out[p] = (both[:, base + 2 * PAIR : base + 3 * PAIR] + term_v).astype(jnp.bfloat16)
        return carry

    lax.fori_loop(0, pairs // 2, project, 0)

    def attend(p, carry):
        cols = pl.ds(pl.multiple_of(p * PAIR, PAIR), PAIR)
        for block in range(tokens // PAIR):
            allowed = allowed_keys(seg_col, seg_row, block)
            rows = slice(block * PAIR, (block + 1) * PAIR)
            window = slice(block * PAIR, block * PAIR + 2 * PAIR)
            query, keys, values = query_out[p, rows, :], key_out[p, window, :], value_out[p, window, :]
            mixed = [
                jnp.dot(probs_of(query, keys, h, allowed).astype(jnp.bfloat16), values, preferred_element_type=jnp.float32)
                for h in range(2)
            ]
            attn[rows, cols] = jnp.where(head_lanes(mixed[0].shape, 0), mixed[0], mixed[1]).astype(jnp.bfloat16)
        return carry

    lax.fori_loop(0, pairs, attend, 0)
    others[0].wait()
    one_out[...] = wide[HALO:, :] + jnp.dot(attn[...], wo[...], preferred_element_type=jnp.float32)

    def second(rows):
        normed_two[rows, :] = layer_norm(one_out[rows, :], gains[1:2, :]).astype(jnp.bfloat16)
        two_out[rows, :] = one_out[rows, :]

    row_blocks(tokens, second)
    others[1].wait()
    others[2].wait()

    def save(c):
        return pltpu.make_async_copy(fc_buf.at[c % 2], fc_out.at[c], fc_sem.at[c % 2])

    def feed(c, carry):
        @pl.when(c >= 2)
        def _():
            save(c - 2).wait()

        inner = jnp.dot(normed_two[...], w1[c], preferred_element_type=jnp.float32)
        fc_buf[c % 2] = inner
        save(c).start()
        two_out[...] += lax.dot_general(
            gelu(inner).astype(jnp.bfloat16), w2[c], NT, preferred_element_type=jnp.float32
        )
        return carry

    lax.fori_loop(0, chunks, feed, 0)
    save(chunks - 2).wait()
    save(chunks - 1).wait()

    def third(rows):
        final = layer_norm(two_out[rows, :], gains[2:3, :]).astype(jnp.bfloat16)
        attn[rows, :] = final
        later = pl.ds(rows.start + reach, rows.size)
        picked = jnp.sum(final.astype(jnp.float32) * emb[later, :].astype(jnp.float32), axis=-1, keepdims=True)
        pick_out[rows, :] = jnp.broadcast_to(picked, (rows.size, pick_out.shape[1]))

    row_blocks(tokens, third)
    place = lax.broadcasted_iota(jnp.int32, (tokens, tokens), 0)
    rows_out[...] = jnp.dot(
        (place == rank_row[...]).astype(jnp.bfloat16), attn[...], preferred_element_type=jnp.float32
    ).astype(jnp.bfloat16)


def forward(emb, pos, seg_col, seg_row, rank_row, gains, down, up_query, up_value, weights):
    wq, wo, w1, w2 = weights
    reach, width = pos.shape
    tokens = reach - HALO
    pairs, chunks, hidden = wq.shape[0], w1.shape[0], w1.shape[2]
    f32, bf16 = jnp.float32, jnp.bfloat16
    vmem, hbm = pl.BlockSpec(memory_space=pltpu.VMEM), pl.BlockSpec(memory_space=pl.ANY)
    return pl.pallas_call(
        forward_kernel,
        out_shape=(
            jax.ShapeDtypeStruct((tokens, width), bf16),
            jax.ShapeDtypeStruct((tokens, 128), f32),
            jax.ShapeDtypeStruct((reach, width), bf16),
            jax.ShapeDtypeStruct((reach, 128), bf16),
            jax.ShapeDtypeStruct((pairs, tokens, PAIR), bf16),
            jax.ShapeDtypeStruct((pairs, reach, PAIR), bf16),
            jax.ShapeDtypeStruct((pairs, reach, PAIR), bf16),
            jax.ShapeDtypeStruct((tokens, width), f32),
            jax.ShapeDtypeStruct((tokens, width), f32),
            jax.ShapeDtypeStruct((chunks, tokens, hidden), f32),
        ),
        in_specs=[vmem] * 9 + [hbm] * 4,
        out_specs=(vmem,) * 9 + (hbm,),
        scratch_shapes=[
            pltpu.VMEM((pairs // 2, width, 6 * PAIR), bf16),
            pltpu.VMEM(wo.shape, bf16),
            pltpu.VMEM(w1.shape, bf16),
            pltpu.VMEM(w2.shape, bf16),
            pltpu.VMEM((reach, width), f32),
            pltpu.VMEM((tokens, width), bf16),
            pltpu.VMEM((tokens, width), bf16),
            pltpu.VMEM((2, tokens, hidden), f32),
            pltpu.SemaphoreType.DMA((pairs,)),
            pltpu.SemaphoreType.DMA((3,)),
            pltpu.SemaphoreType.DMA((2,)),
        ],
        compiler_params=pltpu.CompilerParams(vmem_limit_bytes=VMEM_CAP),
        name="forward",
    )(emb, pos, seg_col, seg_row, rank_row, gains, down, up_query, up_value, wq, wo, w1, w2)


def backward_kernel(
    grad_rows,
    lse_row,
    rank_col,
    pick,
    weight_col,
    target_emb,
    one,
    two,
    gains,
    seg_col,
    seg_row,
    query,
    key,
    value,
    normed,
    low,
    up_query,
    up_value,
    fc_hbm,
    wo_hbm,
    w1_hbm,
    w2_hbm,
    out,
    wo,
    w1,
    w2,
    fc_buf,
    grad_two,
    grad_low,
    grad_inner,
    grad_mixed,
    grad_query,
    grad_value,
    w_sem,
    fc_sem,
):
    tokens, width = two.shape
    pairs, chunks = query.shape[0], w1.shape[0]
    loads = [
        pltpu.make_async_copy(a, b, w_sem.at[i]) for i, (a, b) in enumerate(((w2_hbm, w2), (w1_hbm, w1), (wo_hbm, wo)))
    ]

    def fetch(c):
        return pltpu.make_async_copy(fc_hbm.at[c], fc_buf.at[c % 2], fc_sem.at[c % 2])

    loads[0].start()
    fetch(0).start()
    loads[1].start()
    loads[2].start()

    chosen = rank_col[...] == lax.broadcasted_iota(jnp.int32, (tokens, tokens), 1)
    grad_two[...] = jnp.dot(chosen.astype(jnp.bfloat16), grad_rows[...], preferred_element_type=jnp.float32)
    lse = jnp.sum(jnp.where(chosen, lse_row[...], 0.0), axis=-1, keepdims=True)
    weight = weight_col[...]
    loss = jnp.sum(weight * (lse - pick[:, 0:1]))
    grad_value[0:tokens, 0:128] = jnp.broadcast_to(jnp.exp(pick[:, 0:1] - lse) - 1.0, (tokens, 128))

    def first(rows):
        factor = grad_value[rows, 0:1]
        grad_final = weight_col[rows, :] * (grad_two[rows, :] + factor * target_emb[rows, :].astype(jnp.float32))
        grad = norm_back(two[rows, :], gains[2:3, :], grad_final)
        grad_two[rows, :] = grad
        grad_low[rows, :] = grad.astype(jnp.bfloat16)

    row_blocks(tokens, first)
    grad_inner[...] = jnp.zeros_like(grad_inner)
    for load in loads[:2]:
        load.wait()

    def feed(c, carry):
        fetch(c).wait()

        @pl.when(c + 1 < chunks)
        def _():
            fetch(c + 1).start()

        grad_act = jnp.dot(grad_low[...], w2[c], preferred_element_type=jnp.float32)
        grad_in = (grad_act * gelu_slope(fc_buf[c % 2])).astype(jnp.bfloat16)
        grad_inner[...] += lax.dot_general(grad_in, w1[c], NT, preferred_element_type=jnp.float32)
        return carry

    lax.fori_loop(0, chunks, feed, 0)

    def second(rows):
        grad_one = grad_two[rows, :] + norm_back(one[rows, :], gains[1:2, :], grad_inner[rows, :])
        grad_low[rows, :] = grad_one.astype(jnp.bfloat16)

    row_blocks(tokens, second)
    loads[2].wait()
    grad_mixed[...] = lax.dot_general(grad_low[...], wo[...], NT, preferred_element_type=jnp.float32).astype(jnp.bfloat16)
    grad_value[...] = jnp.zeros_like(grad_value)

    def attend(p, carry):
        cols = pl.ds(pl.multiple_of(p * PAIR, PAIR), PAIR)
        for block in range(tokens // PAIR):
            allowed = allowed_keys(seg_col, seg_row, block)
            rows = slice(block * PAIR, (block + 1) * PAIR)
            window = slice(block * PAIR, block * PAIR + 2 * PAIR)
            keys, values, mixed = key[p, window, :], value[p, window, :], grad_mixed[rows, cols]
            grads_q, grads_v = [], []
            for h in range(2):
                prob = probs_of(query[p, rows, :], keys, h, allowed)
                grad_prob = lax.dot_general(only_head(mixed, h), values, NT, preferred_element_type=jnp.float32)
                inner = jnp.sum(prob * grad_prob, axis=-1, keepdims=True)
                grad_score = (prob * (grad_prob - inner)).astype(jnp.bfloat16)
                grads_q.append(jnp.dot(grad_score, keys, preferred_element_type=jnp.float32) * SCORE_SCALE)
                grads_v.append(lax.dot_general(prob.astype(jnp.bfloat16), mixed, TN, preferred_element_type=jnp.float32))
            grad_query[rows, cols] = jnp.where(head_lanes(grads_q[0].shape, 0), grads_q[0], grads_q[1]).astype(
                jnp.bfloat16
            )
            grad_value[window, cols] += jnp.where(head_lanes(grads_v[0].shape, 0), grads_v[0], grads_v[1])
        return carry

    lax.fori_loop(0, pairs, attend, 0)
    grad_v = grad_value[...].astype(jnp.bfloat16)
    grad_q = grad_query[...]
    low_q = lax.dot_general(grad_q, up_query[...], NT, preferred_element_type=jnp.float32).astype(jnp.bfloat16)
    low_v = lax.dot_general(grad_v, up_value[...], NT, preferred_element_type=jnp.float32).astype(jnp.bfloat16)
    grad_down = lax.dot_general(low_q, normed[HALO:, :], TN, preferred_element_type=jnp.float32)
    grad_down += lax.dot_general(low_v, normed[...], TN, preferred_element_type=jnp.float32)
    up_q = lax.dot_general(low[HALO:, :], grad_q, TN, preferred_element_type=jnp.float32)
    up_v = lax.dot_general(low[...], grad_v, TN, preferred_element_type=jnp.float32)
    out[0:8, :] = grad_down[0:8, :]
    first_rows = lax.broadcasted_iota(jnp.int32, (8, width), 0) < 4
    out[8:16, :] = ADAPTER_SCALE * jnp.where(first_rows, up_q[0:8, :], up_v[0:8, :])
    out[16:24, :] = jnp.broadcast_to(loss, (8, width))


def backward(grad_rows, lse_row, rank_col, pick, weight_col, target_emb, saved, gains, seg_col, seg_row, up_query, up_value, weights):
    normed, low, query, key, value, one, two, fc = saved
    _, wo, w1, w2 = weights
    tokens, width = one.shape
    reach, hidden = normed.shape[0], w1.shape[2]
    f32, bf16 = jnp.float32, jnp.bfloat16
    vmem, hbm = pl.BlockSpec(memory_space=pltpu.VMEM), pl.BlockSpec(memory_space=pl.ANY)
    return pl.pallas_call(
        backward_kernel,
        out_shape=jax.ShapeDtypeStruct((24, width), f32),
        in_specs=[vmem] * 18 + [hbm] * 4,
        out_specs=vmem,
        scratch_shapes=[
            pltpu.VMEM(wo.shape, bf16),
            pltpu.VMEM(w1.shape, bf16),
            pltpu.VMEM(w2.shape, bf16),
            pltpu.VMEM((2, tokens, hidden), f32),
            pltpu.VMEM((tokens, width), f32),
            pltpu.VMEM((tokens, width), bf16),
            pltpu.VMEM((tokens, width), f32),
            pltpu.VMEM((tokens, width), bf16),
            pltpu.VMEM((tokens, width), bf16),
            pltpu.VMEM((reach, width), f32),
            pltpu.SemaphoreType.DMA((3,)),
            pltpu.SemaphoreType.DMA((2,)),
        ],
        compiler_params=pltpu.CompilerParams(vmem_limit_bytes=VMEM_CAP),
        name="backward",
    )(
        grad_rows, lse_row, rank_col, pick, weight_col, target_emb, one, two, gains, seg_col, seg_row,
        query, key, value, normed, low, up_query, up_value, fc, wo, w1, w2,
    )


def finish_kernel(
    src, master, first, second, mask, scalars, stats, new_first, new_second, new_master, new_copy,
    got, squares, squares_got, own_sem, send_sem, recv_sem, send_two, recv_two,
):
    dp, mp = lax.axis_index("dp"), lax.axis_index("mp")
    groups, copies_of = LINE * SIDE, 4
    total = groups * copies_of
    peers = [
        {"dp": lax.rem(dp + k // groups, copies_of), "mp": lax.rem(mp + k % groups, groups)} for k in range(1, total)
    ]
    greet(peers)
    copies = []
    for k in range(1, total):
        copy = remote(
            src.at[lax.rem(mp + k % groups, groups)], got.at[k], send_sem.at[k], recv_sem.at[k], peers[k - 1]
        )
        copy.start()
        copies.append(copy)
    own = pltpu.make_async_copy(src.at[mp], got.at[0], own_sem)
    own.start()
    own.wait()
    grads = got[0]
    for k in range(1, total):
        copies[k - 1].wait_recv()
    for k in range(1, total):
        grads = grads + got[k]
    loss = grads[16:24, :]
    grads = grads[0:16, :]
    squares[...] = jnp.broadcast_to(jnp.sum(grads * grads), squares.shape)
    again = []
    for k in range(1, groups):
        copy = remote(squares, squares_got.at[k], send_two.at[k], recv_two.at[k], peers[k - 1])
        copy.start()
        again.append(copy)
    for copy in again:
        copy.wait()
    square_sum = squares[...]
    for k in range(1, groups):
        square_sum = square_sum + squares_got[k]
    norm = jnp.sqrt(square_sum)
    stats[0] = loss
    stats[1] = norm
    clipped = grads * jnp.minimum(1.0, CLIP_NORM / (norm[0:1, :] + 1e-06))
    one = BETA_ONE * first[...] + (1.0 - BETA_ONE) * clipped
    two = BETA_TWO * second[...] + (1.0 - BETA_TWO) * clipped * clipped
    one_hat = one / scalars[0:1, :]
    two_hat = two / scalars[1:2, :]
    weight = master[...] - LEARN_RATE * (one_hat / (jnp.sqrt(two_hat) + ADAM_EPS) + WEIGHT_DECAY * master[...])
    keep = mask[...]
    new_first[...] = keep * one
    new_second[...] = keep * two
    new_master[...] = keep * weight
    new_copy[...] = (keep * weight).astype(jnp.bfloat16)
    for copy in copies:
        copy.wait_send()


def finish(grads, master, first, second, mask, scalars, collective):
    groups = lax.axis_size("mp")
    width = grads.shape[1]
    cols = width // groups
    slices = jnp.transpose(grads.reshape(24, groups, cols), (1, 0, 2))
    if not is_own_mesh():
        summed = lax.psum(lax.psum_scatter(slices, "mp", scatter_dimension=0), "dp")
        owned = summed[:16]
        norm = jnp.sqrt(lax.psum(jnp.sum(owned * owned), "mp"))
        clipped = owned * jnp.minimum(1.0, CLIP_NORM / (norm + 1e-06))
        one = BETA_ONE * first + (1.0 - BETA_ONE) * clipped
        two = BETA_TWO * second + (1.0 - BETA_TWO) * clipped * clipped
        weight = master - LEARN_RATE * (
            one / scalars[0, 0] / (jnp.sqrt(two / scalars[1, 0]) + ADAM_EPS) + WEIGHT_DECAY * master
        )
        kept = mask * weight
        return summed[16, 0], norm, mask * one, mask * two, kept, kept.astype(jnp.bfloat16)
    vmem = pl.BlockSpec(memory_space=pltpu.VMEM)
    tile = jax.ShapeDtypeStruct((16, cols), jnp.float32)
    total = groups * 4
    stats, one, two, weight, copy = pl.pallas_call(
        finish_kernel,
        out_shape=(jax.ShapeDtypeStruct((2, 8, cols), jnp.float32), tile, tile, tile, jax.ShapeDtypeStruct((16, cols), jnp.bfloat16)),
        in_specs=[vmem] * 6,
        out_specs=(vmem,) * 5,
        scratch_shapes=[
            pltpu.VMEM((total, 24, cols), jnp.float32),
            pltpu.VMEM((8, cols), jnp.float32),
            pltpu.VMEM((groups, 8, cols), jnp.float32),
            pltpu.SemaphoreType.DMA,
            pltpu.SemaphoreType.DMA((total,)),
            pltpu.SemaphoreType.DMA((total,)),
            pltpu.SemaphoreType.DMA((groups,)),
            pltpu.SemaphoreType.DMA((groups,)),
        ],
        compiler_params=pltpu.CompilerParams(collective_id=collective, has_side_effects=True),
        name="finish",
    )(slices, master, first, second, mask, scalars)
    return stats[0, 0, 0], stats[1, 0, 0], one, two, weight, copy


ROUND_ROWS = 80


def fetch_rows(embedding, ids, parts, tokens, collective):
    groups, mine = lax.axis_size("mp"), lax.axis_index("mp")
    vocab_local, width = embedding.shape
    seq = ids.shape[1]
    reach = HALO + tokens
    window = reach + 8
    spots = jnp.arange(parts)[:, None] * tokens - HALO + jnp.arange(window)[None, :]
    spots = jnp.clip(spots, 0, seq - 1)
    wanted = ids[:, spots].reshape(groups, window)
    holder = wanted // vocab_local
    if not is_own_mesh():
        near = wanted - mine * vocab_local
        inside = (near >= 0) & (near < vocab_local)
        rows = jnp.where(inside[..., None], jnp.take(embedding, jnp.clip(near, 0, vocab_local - 1), axis=0), 0)
        rows = lax.psum_scatter(rows, "mp", scatter_dimension=0)
        rows = jnp.concatenate([rows[:reach], rows[HALO + 1 : HALO + 1 + tokens]], axis=0)
        return jnp.float32(0.0), lambda rounds: rows
    earlier = jnp.arange(window)[:, None] > jnp.arange(window)[None, :]
    same = wanted[:, :, None] == wanted[:, None, :]
    lead = jnp.logical_not(jnp.any(same & earlier[None], axis=2))
    below = (holder[:, :, None] == holder[:, None, :]) & (wanted[:, None, :] < wanted[:, :, None]) & lead[:, None, :]
    slot = jnp.sum(below.astype(jnp.int32), axis=2)
    need = (jnp.max(slot) + 1).astype(jnp.float32)
    asked = lead & (holder == mine)
    my_slot = lax.dynamic_index_in_dim(slot, mine, 0, keepdims=False)
    my_holder = lax.dynamic_index_in_dim(holder, mine, 0, keepdims=False)

    def listed(values):
        return jnp.concatenate([values[:reach], values[HALO + 1 : HALO + 1 + tokens]])

    list_slot, list_holder = listed(my_slot), listed(my_holder)

    def one_round(r):
        base = r * ROUND_ROWS
        hit = asked[:, None, :] & (slot[:, None, :] == base + jnp.arange(ROUND_ROWS)[None, :, None])
        chosen = jnp.sum(jnp.where(hit, wanted[:, None, :] - mine * vocab_local, 0), axis=2)
        rows = jnp.take(embedding, chosen.reshape(-1), axis=0, mode="clip").reshape(groups, ROUND_ROWS, width)
        got = swap(rows, True, collective).reshape(groups * ROUND_ROWS, width)
        place = list_slot - base
        place = jnp.where((place >= 0) & (place < ROUND_ROWS), list_holder * ROUND_ROWS + place, -1)
        pick = (place[:, None] == jnp.arange(groups * ROUND_ROWS)[None, :]).astype(jnp.bfloat16)
        return jnp.dot(pick, got, preferred_element_type=jnp.float32).astype(jnp.bfloat16)

    def all_rounds(rounds):
        def lap(state):
            r, so_far = state
            return r + 1, so_far + one_round(r)

        return lax.while_loop(lambda state: state[0] < rounds, lap, (jnp.int32(1), one_round(jnp.int32(0))))[1]

    return need, all_rounds


def local(
    packed_token_rows,
    example_numbers,
    completion,
    global_token_count,
    owners,
    optimizer_step,
    embedding,
    positions,
    gains,
    query_key_value_weight,
    attention_output_weight,
    feedforward_input_weight,
    feedforward_output_weight,
    adapter_down_weight,
    adapter_up_weight,
    master,
    first_moment,
    second_moment,
):
    groups, mine = lax.axis_size("mp"), lax.axis_index("mp")
    batch, seq = packed_token_rows.shape
    width = embedding.shape[1]
    vocab_local = embedding.shape[0]
    tokens = batch * seq // groups
    parts = seq // tokens
    reach = HALO + tokens
    row, part = mine // parts, mine % parts
    start = part * tokens
    rank_size = adapter_down_weight.shape[1]
    pairs = width // PAIR
    head_cols = query_key_value_weight.shape[2]

    places = jnp.arange(seq, dtype=jnp.int32)
    is_valid = (
        (places[None, :] < seq - 1)
        & (jnp.roll(example_numbers, -1, axis=1) == example_numbers)
        & (jnp.roll(completion, -1, axis=1) == 1)
    ).reshape(groups, tokens)
    before = (jnp.arange(tokens)[:, None] < jnp.arange(tokens)[None, :]).astype(jnp.bfloat16)
    rank = jnp.dot(is_valid.astype(jnp.bfloat16), before, preferred_element_type=jnp.float32).astype(jnp.int32)
    rank = jnp.where(is_valid, rank, -1)
    targets = jnp.roll(packed_token_rows, -1, axis=1).reshape(groups, tokens)
    need_rows = jnp.max(jnp.sum(is_valid.astype(jnp.float32), axis=1))

    need_slots, all_rounds = fetch_rows(embedding, packed_token_rows, parts, tokens, 1)
    agreed = agree(jnp.stack([need_slots, need_rows]), 2)
    rounds = ((agreed[0].astype(jnp.int32) + ROUND_ROWS - 1) // ROUND_ROWS).astype(jnp.int32)
    emb = all_rounds(rounds)

    wq = query_key_value_weight.reshape(width, 3 * head_cols)
    up_rows = adapter_up_weight.reshape(2 * rank_size, head_cols)
    if is_own_mesh():
        extra = jnp.pad(up_rows, ((0, 64 - 2 * rank_size), (0, 2 * head_cols)))
        wq = jnp.concatenate([wq, extra], axis=0)
        wq, wo, w1, w2 = gather_weights(
            [wq, attention_output_weight, feedforward_input_weight, feedforward_output_weight], 3
        )
        up_all = jnp.transpose(wq[:, width : width + 2 * rank_size, :head_cols], (1, 0, 2))
    else:
        wq, wo, w1, w2, up_all = gather_weights(
            [wq, attention_output_weight, feedforward_input_weight, feedforward_output_weight, up_rows], 3
        )
        wq = jnp.transpose(wq.reshape(groups, width, 3, head_cols), (1, 2, 0, 3)).reshape(width, 3, pairs, PAIR)
        wq = jnp.transpose(wq, (2, 0, 1, 3)).reshape(pairs, width, 3 * PAIR)
        up_all = jnp.transpose(up_all, (1, 0, 2))
    wo = wo.reshape(width, width)
    weights = (wq, wo, w1, w2)
    up_all = (ADAPTER_SCALE * up_all.reshape(2 * rank_size, width).astype(jnp.float32)).astype(jnp.bfloat16)
    up_query = jnp.pad(up_all[:rank_size], ((0, 128 - rank_size), (0, 0)))
    up_value = jnp.pad(up_all[rank_size:], ((rank_size, 128 - 2 * rank_size), (0, 0)))
    down = jnp.pad(adapter_down_weight.reshape(2 * rank_size, width), ((0, 128 - 2 * rank_size), (0, 0)))

    def window_of(values):
        first = lax.dynamic_slice_in_dim(values, jnp.maximum(start - HALO, 0), HALO, 0)
        return jnp.concatenate([first, lax.dynamic_slice_in_dim(values, start, tokens, 0)], axis=0)

    pos = window_of(positions)
    seg = window_of(lax.dynamic_index_in_dim(example_numbers, row, 0, keepdims=False))
    seg = jnp.where((jnp.arange(reach) < HALO) & (part == 0), -1, seg)
    my_rank = lax.dynamic_index_in_dim(rank, mine, 0, keepdims=False)
    my_valid = (my_rank >= 0).astype(jnp.float32)
    seg_col, seg_row = seg[:, None], seg[None, :]
    rows_c, pick, normed, low, query, key, value, one, two, fc = forward(
        emb, pos, seg_col, seg_row, my_rank[None, :], gains, down, up_query, up_value, weights
    )

    def wanted_of(first, count):
        spot = rank[:, None, :] == first + jnp.arange(count, dtype=jnp.int32)[None, :, None]
        return (jnp.sum(jnp.where(spot, targets[:, None, :], 0), axis=2) - mine * vocab_local)[:, :, None]

    def head_plain(first, count, collective):
        everyone = spread(rows_c[first : first + count], collective).reshape(groups * count, width)
        grad, total = head(everyone, wanted_of(first, count).reshape(groups * count, 1), embedding)
        total = total[:, 0].reshape(groups, count)
        if is_own_mesh():
            lanes = -(-count // 128) * 128
            totals = swap(jnp.pad(total, ((0, 0), (0, lanes - count))), False, collective + 1)[:, :, :count]
        else:
            totals = lax.all_gather(total, "mp", axis=0)
        peak = jnp.max(totals, axis=0)
        lse = peak + jnp.log(jnp.sum(jnp.exp(totals - peak[None]), axis=0))
        grad = grad.reshape(groups, count, width) * jnp.exp(total - lse)[:, :, None]
        summed = collect(grad.astype(jnp.bfloat16), collective + 2)
        return summed, lax.dynamic_index_in_dim(lse, mine, 0, keepdims=False)

    if is_own_mesh():
        count = tokens * 9 // 16
        rest = tokens - count
        more_rows, more_lse = lax.cond(
            agreed[1] > count,
            lambda: head_plain(count, rest, 4),
            lambda: (jnp.zeros((rest, width), jnp.bfloat16), jnp.zeros((rest,), jnp.float32)),
        )
        grad_rows, lse_tile = head_all(rows_c[:count], wanted_of(0, count), embedding, 7)
        grad_rows = jnp.concatenate([grad_rows, more_rows], axis=0)
        lse = jnp.concatenate([lse_tile[0, :count], more_lse])
    else:
        grad_rows, lse = head_plain(0, tokens, 4)

    weight_col = (my_valid / global_token_count.astype(jnp.float32))[:, None]
    grads = backward(
        grad_rows, lse[None, :], my_rank[:, None], pick, weight_col, emb[reach:],
        (normed, low, query, key, value, one, two, fc), gains, seg_col, seg_row, up_query, up_value, weights,
    )

    dp_index = lax.axis_index("dp")
    cols = master.shape[2]
    flat = (4 * rank_size, cols)
    mask = jnp.broadcast_to((owners == dp_index).astype(jnp.float32).reshape(4 * rank_size, 1), flat)
    step = optimizer_step.astype(jnp.float32)
    scalars = jnp.stack([1.0 - jnp.power(BETA_ONE, step), 1.0 - jnp.power(BETA_TWO, step)])
    scalars = jnp.broadcast_to(jnp.pad(scalars, (0, 6))[:, None], (8, cols))
    loss, norm, new_first, new_second, new_master, new_copy = finish(
        grads, master.reshape(flat), first_moment.reshape(flat), second_moment.reshape(flat), mask, scalars, 13
    )
    shape = (1,) + master.shape
    return (
        loss,
        norm,
        new_first.reshape(shape),
        new_second.reshape(shape),
        new_master.reshape(shape),
        new_copy.reshape(shape),
    )


def solution(mesh):
    return jax.shard_map(
        local,
        mesh=mesh,
        in_specs=(
            P("dp", None),
            P("dp", None),
            P("dp", None),
            P(),
            P(),
            P(),
            P("mp", None),
            P(),
            P(),
            P(None, None, "mp"),
            P("mp", None),
            P(None, "mp"),
            P(None, "mp"),
            P(),
            P(None, None, "mp"),
            P(None, None, "mp"),
            P(None, None, "mp"),
            P(None, None, "mp"),
        ),
        out_specs=(
            P(),
            P(),
            P("dp", None, None, "mp"),
            P("dp", None, None, "mp"),
            P("dp", None, None, "mp"),
            P("dp", None, None, "mp"),
        ),
        check_vma=False,
    )
```
